512 devices in a mesh: row: 16 (over z), col: 16 (over y, x), layer: 2 (over core).
Axes of the slice: x: 4, y: 4, z: 16, core: 2. Of those that a mesh axis runs over, the one named last changes fastest.
Arguments:
- ratings: bfloat16 [32768, 16384], P('row', ('col', 'layer')), may hold values from -6 to 6
- tile_mask: int32 [256, 128], P('row', ('col', 'layer')), may hold values 0 or 1
- tile_counts: int32 [256, 128], P('row', ('col', 'layer')), may hold values from 1 to 16384
- user_factor: float32 [256, 32768], P(('col', 'layer'), 'row'), may hold values from -1.5 to 1.5
- item_factor: float32 [256, 16384], P('row', ('col', 'layer')), may hold values from -1.5 to 1.5
Outputs:
- new_user: float32 [256, 32768], P(('col', 'layer'), 'row')
- new_item: float32 [256, 16384], P('row', ('col', 'layer'))
- loss_value: float32 [], replicated
- grad_norm: float32 [], replicated
The draws below stay inside these ranges and needn't reach their ends.
All inputs are finite; a program needn't handle non-finite values. No bound on the sum of `tile_mask` on one device may be relied on, other than what follows from the above.
Results may differ from the reference program's by a relative error of at most 0.0049.
Values may be sent and summed in bfloat16 or wider, within the bound.
No kernel may reach another device: no remote copies, remote signals or barrier semaphores. Data moves between devices by JAX's collectives and lax.ppermute only.
A program may use at most 64 MiB of HBM per device.

```python
import jax
import jax.numpy as jnp
from jax import lax

K = 256
TILE = 128
BR = 2048
NR = 32768
NC = 16384


def place_ends(result, stream_key, least, high):
    extent = result.shape
    spot = [jax.random.randint(jax.random.fold_in(stream_key, axis), (), 0, extent[axis]) for axis in range(len(extent))]
    result = result.at[tuple(spot)].set(least)
    longest = extent.index(max(extent))
    spot[longest] = (spot[longest] + 1) % extent[longest]
    return result.at[tuple(spot)].set(high)


def level_of(key, dims, cuts, least, high):
    factor_of, own = 1.0, jax.random.fold_in(key, 6)
    for axis_at, shards_of in cuts:
        heights = jnp.exp(jax.random.uniform(jax.random.fold_in(own, axis_at), (shards_of,), jnp.float32, least / len(cuts), high / len(cuts)))
        factor_of = factor_of * jnp.repeat(heights, dims[axis_at] // shards_of).reshape([-1 if axis == axis_at else 1 for axis in range(len(dims))])
    return factor_of


def gaussian(key, shape, spread, limit, split=(), dtype=jnp.bfloat16):
    drawn = jax.random.normal(key, shape, jnp.float32) * spread
    if len(split) > 0:
        drawn = level_of(key, shape, split, -0.22, 0.18) * drawn
    return jnp.clip(drawn, min=-limit, max=limit).astype(dtype)


def setup_inputs(seed: int = 0) -> dict:
    splits = jax.random.split(jax.random.key(seed), 6)
    return {
        "ratings": gaussian(splits[0], (NR, NC), 1.0, 6.0, ((0, 16), (1, 32))),
        "tile_mask": place_ends((jax.random.randint(splits[1], (NR // TILE, NC // TILE), 0, 4) < 3).astype(jnp.int32), jax.random.fold_in(splits[1], 1), 0, 1),
        "tile_counts": place_ends(jax.random.randint(splits[2], (NR // TILE, NC // TILE), 1, TILE * TILE + 1), jax.random.fold_in(splits[2], 1), 1, TILE * TILE).astype(jnp.int32),
        "user_factor": gaussian(splits[3], (K, NR), 0.25, 1.5, ((0, 32), (1, 16)), jnp.float32),
        "item_factor": gaussian(splits[4], (K, NC), 0.25, 1.5, ((0, 16), (1, 32)), jnp.float32),
    }


epsilon = 1e-12
trust_ratio = 0.2

def tile_weights(mask_rows, count_rows):
    position = lax.broadcasted_iota(jnp.int32, (TILE, TILE), 0) * TILE + lax.broadcasted_iota(jnp.int32, (TILE, TILE), 1)
    observed = (mask_rows[:, None, :, None] == 1) & (position[None, :, None, :] < count_rows[:, None, :, None])
    return observed.astype(jnp.float32).reshape(mask_rows.shape[0] * TILE, mask_rows.shape[1] * TILE)

def reference(ratings, tile_mask, tile_counts, user_factor, item_factor):
    user_low = user_factor.astype(jnp.bfloat16)
    item_low = item_factor.astype(jnp.bfloat16)
    observed_total = jnp.maximum(jnp.sum(tile_mask * tile_counts).astype(jnp.float32), jnp.float32(1.0))
    blocks = NR // BR

    def advance(running, block_index):
        error_sum, raw_item = running
        offset = (block_index * BR).astype(jnp.int32)
        tile_offset = (block_index * (BR // TILE)).astype(jnp.int32)
        rating_rows = lax.dynamic_slice_in_dim(ratings, offset, BR, 0)
        mask_rows = lax.dynamic_slice_in_dim(tile_mask, tile_offset, BR // TILE, 0)
        count_rows = lax.dynamic_slice_in_dim(tile_counts, tile_offset, BR // TILE, 0)
        user_rows = lax.dynamic_slice_in_dim(user_low, offset, BR, 1)
        predicted = lax.dot_general(user_rows, item_low, (((0,), (0,)), ((), ())), preferred_element_type=jnp.float32)
        residual = tile_weights(mask_rows, count_rows) * (predicted - rating_rows.astype(jnp.float32))
        scaled = residual.astype(jnp.bfloat16)
        raw_user = lax.dot_general(item_low, scaled, (((1,), (1,)), ((), ())), preferred_element_type=jnp.float32)
        raw_item = raw_item + jnp.dot(user_rows, scaled, preferred_element_type=jnp.float32)
        return ((error_sum + jnp.sum(residual * residual), raw_item), raw_user)
    start_state = (jnp.float32(0.0), jnp.zeros((K, NC), jnp.float32))
    (error_sum, raw_item), user_blocks = lax.scan(advance, start_state, jnp.arange(blocks).astype(jnp.int32))
    raw_user = jnp.transpose(user_blocks, (1, 0, 2)).reshape(K, NR)
    loss_value = error_sum / observed_total
    grad_norm = 2.0 / observed_total * jnp.sqrt(jnp.sum(raw_user * raw_user) + jnp.sum(raw_item * raw_item) + epsilon)
    factor_norm = jnp.sqrt(jnp.sum(user_factor * user_factor) + jnp.sum(item_factor * item_factor) + epsilon)
    rate = trust_ratio * factor_norm / grad_norm
    step_size = rate * (2.0 / observed_total)
    new_user = user_factor - step_size * raw_user
    new_item = item_factor - step_size * raw_item
    return (new_user, new_item, loss_value, grad_norm)
```

```python
import jax
import jax.numpy as jnp
from jax import lax
from jax.sharding import Mesh
from jax.sharding import PartitionSpec as P

TILE = 128
COL_LAYER = ("col_0", "col_1", "layer")


epsilon = 1e-12
trust_ratio = 0.2


def from_everyone(array, axis):
    count = lax.axis_size(axis)
    return lax.all_to_all(
        jnp.broadcast_to(array[None], (count, *array.shape)), axis, 0, 0, tiled=True
    )


def joined_along(blocks, dim):
    dims = list(blocks.shape[1:])
    dims[dim] *= blocks.shape[0]
    return jnp.moveaxis(blocks, 0, dim).reshape(dims)


def gather_directly(array, axis, dim):
    blocks = from_everyone(array, axis)
    return joined_along(blocks, dim)


def in_blocks(array, dim, count):
    dims = array.shape
    blocks = array.reshape(*dims[:dim], count, dims[dim] // count, *dims[dim + 1 :])
    return jnp.moveaxis(blocks, dim, 0)


def sent(array, axis, dim):
    blocks = in_blocks(array, dim, lax.axis_size(axis))
    return lax.all_to_all(blocks, axis, split_axis=0, concat_axis=0, tiled=True)


def summed(arrived):
    return arrived.astype(jnp.float32).sum(axis=0)


def tile_weights(mask_rows, count_rows):
    side = TILE
    position = lax.broadcasted_iota(jnp.int32, (side, side), 0) * side + lax.broadcasted_iota(
        jnp.int32, (side, side), 1
    )
    observed = (mask_rows[:, None, :, None] == 1) & (
        position[None, :, None, :] < count_rows[:, None, :, None]
    )
    return observed.astype(jnp.float32).reshape(
        mask_rows.shape[0] * side, mask_rows.shape[1] * side
    )


def scalars_summed(scalars):
    packed = jnp.stack(scalars + [jnp.float32(0.0)] * (TILE - len(scalars)))[None]
    packed = from_everyone(packed, COL_LAYER).sum(axis=0)
    packed = from_everyone(packed, "row").sum(axis=0)
    return [packed[0, i] for i in range(len(scalars))]


def body(ratings, tile_mask, tile_counts, user_factor, item_factor):
    user_low = user_factor.astype(jnp.bfloat16)
    item_low = item_factor.astype(jnp.bfloat16)
    item_cols = gather_directly(item_low, "row", 0)
    user_rows = gather_directly(user_low, COL_LAYER, 0)
    count_local = jnp.sum(tile_mask * tile_counts).astype(jnp.float32)
    factor_local = jnp.sum(user_factor * user_factor) + jnp.sum(item_factor * item_factor)
    predicted = lax.dot_general(
        user_rows, item_cols, (((0,), (0,)), ((), ())), preferred_element_type=jnp.float32
    )
    residual = tile_weights(tile_mask, tile_counts) * (predicted - ratings.astype(jnp.float32))
    scaled = residual.astype(jnp.bfloat16)
    error_local = jnp.sum(residual * residual)
    item_share = jnp.dot(user_rows, scaled, preferred_element_type=jnp.float32)
    item_arrived = sent(item_share.astype(jnp.bfloat16), "row", 0)
    user_share = lax.dot_general(
        item_cols, scaled, (((1,), (1,)), ((), ())), preferred_element_type=jnp.float32
    )
    user_arrived = sent(user_share.astype(jnp.bfloat16), COL_LAYER, 0)
    raw_item = summed(item_arrived)
    raw_user = summed(user_arrived)
    gradient_local = jnp.sum(raw_user * raw_user) + jnp.sum(raw_item * raw_item)
    count_sum, factor_sum, error_sum, gradient_sum = scalars_summed(
        [count_local, factor_local, error_local, gradient_local]
    )
    observed_total = jnp.maximum(count_sum, jnp.float32(1.0))
    loss_value = error_sum / observed_total
    grad_norm = 2.0 / observed_total * jnp.sqrt(gradient_sum + epsilon)
    factor_norm = jnp.sqrt(factor_sum + epsilon)
    rate = trust_ratio * factor_norm / grad_norm
    step_size = rate * (2.0 / observed_total)
    new_user = user_factor - step_size * raw_user
    new_item = item_factor - step_size * raw_item
    return (new_user, new_item, loss_value, grad_norm)


def solution(mesh):
    finer = Mesh(
        mesh.devices.reshape(mesh.shape["row"], 4, 4, mesh.shape["layer"]),
        ("row", "col_0", "col_1", "layer"),
    )
    return jax.shard_map(
        body,
        mesh=finer,
        in_specs=(
            P("row", COL_LAYER),
            P("row", COL_LAYER),
            P("row", COL_LAYER),
            P(COL_LAYER, "row"),
            P("row", COL_LAYER),
        ),
        out_specs=(P(COL_LAYER, "row"), P("row", COL_LAYER), P(), P()),
        check_vma=False,
    )
```

```python
import jax
import jax.numpy as jnp
from jax import lax
from jax.sharding import Mesh
from jax.sharding import PartitionSpec as P

TILE = 128
COL_LAYER = ("col_0", "col_1", "layer")


epsilon = 1e-12
trust_ratio = 0.2


def from_everyone(array, axis):
    count = lax.axis_size(axis)
    return lax.all_to_all(
        jnp.broadcast_to(array[None], (count, *array.shape)), axis, 0, 0, tiled=True
    )


def joined_along(blocks, dim):
    dims = list(blocks.shape[1:])
    dims[dim] *= blocks.shape[0]
    return jnp.moveaxis(blocks, 0, dim).reshape(dims)


def gather_directly(array, axis, dim):
    blocks = from_everyone(array, axis)
    return joined_along(blocks, dim)


def in_blocks(array, dim, count):
    dims = array.shape
    blocks = array.reshape(*dims[:dim], count, dims[dim] // count, *dims[dim + 1 :])
    return jnp.moveaxis(blocks, dim, 0)


def sent(array, axis, dim):
    blocks = in_blocks(array, dim, lax.axis_size(axis))
    return lax.all_to_all(blocks, axis, split_axis=0, concat_axis=0, tiled=True)


def summed(arrived):
    return arrived.astype(jnp.float32).sum(axis=0)


def tile_weights(mask_rows, count_rows):
    side = TILE
    position = lax.broadcasted_iota(jnp.int32, (side, side), 0) * side + lax.broadcasted_iota(
        jnp.int32, (side, side), 1
    )
    observed = (mask_rows[:, None, :, None] == 1) & (
        position[None, :, None, :] < count_rows[:, None, :, None]
    )
    return observed.astype(jnp.float32).reshape(
        mask_rows.shape[0] * side, mask_rows.shape[1] * side
    )


def scalars_summed(scalars):
    packed = jnp.stack(scalars + [jnp.float32(0.0)] * (TILE - len(scalars)))[None]
    packed = from_everyone(packed, COL_LAYER).sum(axis=0)
    packed = from_everyone(packed, "row").sum(axis=0)
    return [packed[0, i] for i in range(len(scalars))]


def body(ratings, tile_mask, tile_counts, user_factor, item_factor):
    user_low = user_factor.astype(jnp.bfloat16)
    item_low = item_factor.astype(jnp.bfloat16)
    item_cols = gather_directly(item_low, "row", 0)
    user_rows = lax.all_gather(user_low, COL_LAYER, axis=0, tiled=True)
    count_local = jnp.sum(tile_mask * tile_counts).astype(jnp.float32)
    factor_local = jnp.sum(user_factor * user_factor) + jnp.sum(item_factor * item_factor)
    predicted = lax.dot_general(
        user_rows, item_cols, (((0,), (0,)), ((), ())), preferred_element_type=jnp.float32
    )
    residual = tile_weights(tile_mask, tile_counts) * (predicted - ratings.astype(jnp.float32))
    scaled = residual.astype(jnp.bfloat16)
    error_local = jnp.sum(residual * residual)
    item_share = jnp.dot(user_rows, scaled, preferred_element_type=jnp.float32)
    item_arrived = sent(item_share.astype(jnp.bfloat16), "row", 0)
    user_share = lax.dot_general(
        item_cols, scaled, (((1,), (1,)), ((), ())), preferred_element_type=jnp.float32
    )
    raw_user = lax.psum_scatter(
        user_share.astype(jnp.bfloat16), COL_LAYER, scatter_dimension=0, tiled=True
    ).astype(jnp.float32)
    raw_item = summed(item_arrived)
    gradient_local = jnp.sum(raw_user * raw_user) + jnp.sum(raw_item * raw_item)
    count_sum, factor_sum, error_sum, gradient_sum = scalars_summed(
        [count_local, factor_local, error_local, gradient_local]
    )
    observed_total = jnp.maximum(count_sum, jnp.float32(1.0))
    loss_value = error_sum / observed_total
    grad_norm = 2.0 / observed_total * jnp.sqrt(gradient_sum + epsilon)
    factor_norm = jnp.sqrt(factor_sum + epsilon)
    rate = trust_ratio * factor_norm / grad_norm
    step_size = rate * (2.0 / observed_total)
    new_user = user_factor - step_size * raw_user
    new_item = item_factor - step_size * raw_item
    return (new_user, new_item, loss_value, grad_norm)


def solution(mesh):
    finer = Mesh(
        mesh.devices.reshape(mesh.shape["row"], 4, 4, mesh.shape["layer"]),
        ("row", "col_0", "col_1", "layer"),
    )
    return jax.shard_map(
        body,
        mesh=finer,
        in_specs=(
            P("row", COL_LAYER),
            P("row", COL_LAYER),
            P("row", COL_LAYER),
            P(COL_LAYER, "row"),
            P("row", COL_LAYER),
        ),
        out_specs=(P(COL_LAYER, "row"), P("row", COL_LAYER), P(), P()),
        check_vma=False,
    )
```

```python
import jax
import jax.numpy as jnp
from jax import lax
from jax.experimental import pallas as pl
from jax.experimental.pallas import tpu as pltpu
from jax.sharding import Mesh
from jax.sharding import PartitionSpec as P

TILE = 128
LANES = 128
STRIPE = 256
COL_LAYER = ("col_0", "col_1", "layer")
VMEM = pl.BlockSpec(memory_space=pltpu.VMEM)
SMEM = pl.BlockSpec(memory_space=pltpu.SMEM)
ANYWHERE = pl.BlockSpec(memory_space=pl.ANY)
GRANT = pltpu.CompilerParams(vmem_limit_bytes=16 * 2**20)

epsilon = 1e-12
trust_ratio = 0.2


def turned_by_core(pair, layer):
    half = pair.shape[-2] // 2
    swapped = jnp.concatenate([pair[half:], pair[:half]], axis=0)
    return jnp.where(layer == 1, swapped, pair)


def lower_body(layer_ref, user_ref, item_ref, user_low_ref, item_blocks_ref):
    user_low_ref[...] = user_ref[...].astype(jnp.bfloat16)
    item = turned_by_core(item_ref[...], layer_ref[0]).astype(jnp.bfloat16)
    item_blocks_ref[...] = jnp.broadcast_to(item[None], item_blocks_ref.shape)


def lowered(layer, user_factor, item_factor, rows):
    return pl.pallas_call(
        lower_body,
        in_specs=[SMEM, VMEM, VMEM],
        out_specs=[VMEM, VMEM],
        out_shape=[
            jax.ShapeDtypeStruct(user_factor.shape, jnp.bfloat16),
            jax.ShapeDtypeStruct((rows, *item_factor.shape), jnp.bfloat16),
        ],
        compiler_params=GRANT,
        name="lower",
    )(layer, user_factor, item_factor)


def own_halves_first(blocks):
    count, pair, columns = blocks.shape
    halves = [blocks[:, : pair // 2], blocks[:, pair // 2 :]]
    return jnp.concatenate([half.reshape(count * pair // 2, columns) for half in halves], axis=0)


def residual_body(
    mask_ref, counts_ref, mine_ref, other_ref, item_blocks_ref, far_ratings_ref,
    scaled_ref, item_share_ref, item_ref, error_ref, user_ref, ratings_ref, total_ref, user_sems, ratings_sems,
):
    rank_half = mine_ref.shape[0]
    user_copies = [
        pltpu.make_async_copy(half_ref, user_ref.at[pl.ds(at * rank_half, rank_half)], user_sems.at[at])
        for at, half_ref in enumerate((mine_ref, other_ref))
    ]
    stripes = range(0, ratings_ref.shape[0], STRIPE)
    ratings_copies = [
        pltpu.make_async_copy(
            far_ratings_ref.at[pl.ds(start, STRIPE)], ratings_ref.at[pl.ds(start, STRIPE)], ratings_sems.at[at]
        )
        for at, start in enumerate(stripes)
    ]
    for copy in user_copies + ratings_copies:
        copy.start()
    item_ref[...] = own_halves_first(item_blocks_ref[...])
    item = item_ref[...]
    for copy in user_copies:
        copy.wait()
    side = (TILE, TILE)
    position = lax.broadcasted_iota(jnp.int32, side, 0) * TILE + lax.broadcasted_iota(jnp.int32, side, 1)
    columns = ratings_ref.shape[1]
    for start, copy in zip(stripes, ratings_copies):
        stripe = pl.ds(start, STRIPE)
        user = user_ref[:, stripe]
        predicted = lax.dot_general(user, item, (((0,), (0,)), ((), ())), preferred_element_type=jnp.float32)
        copy.wait()
        for row in range(0, STRIPE, TILE):
            for column in range(0, columns, TILE):
                tile_at = (column // TILE, (start + row) // TILE)
                limit = jnp.where(mask_ref[tile_at] == 1, counts_ref[tile_at], 0)
                rows, cols = pl.ds(start + row, TILE), pl.ds(column, TILE)
                difference = predicted[row : row + TILE, column : column + TILE] - ratings_ref[rows, cols].astype(
                    jnp.float32
                )
                residual = jnp.where(position < limit, difference, 0.0)
                scaled_ref[rows, cols] = residual.astype(jnp.bfloat16)
                error = (residual * residual).reshape(TILE // 8, 8, TILE).sum(axis=0)
                if start + row == 0:
                    error_ref[:, cols] = error
                else:
                    error_ref[:, cols] += error
        share = jnp.dot(user, scaled_ref[stripe], preferred_element_type=jnp.float32)
        if start == 0:
            total_ref[...] = share
        else:
            total_ref[...] += share
    count, pair, _ = item_share_ref.shape
    half = pair // 2
    share = total_ref[...].astype(jnp.bfloat16)
    for part in range(2):
        rows = share[part * rank_half : (part + 1) * rank_half]
        item_share_ref[:, part * half : (part + 1) * half] = rows.reshape(count, half, columns)


def residual_of(mask, counts, mine, other, item_blocks, ratings):
    rank, columns = 2 * mine.shape[0], ratings.shape[1]
    flops = 4 * rank * ratings.shape[0] * columns
    return pl.pallas_call(
        residual_body,
        in_specs=[SMEM, SMEM, ANYWHERE, ANYWHERE, VMEM, ANYWHERE],
        out_specs=[VMEM] * 4,
        out_shape=[
            jax.ShapeDtypeStruct(ratings.shape, jnp.bfloat16),
            jax.ShapeDtypeStruct(item_blocks.shape, jnp.bfloat16),
            jax.ShapeDtypeStruct((rank, columns), jnp.bfloat16),
            jax.ShapeDtypeStruct((8, columns), jnp.float32),
        ],
        scratch_shapes=[
            pltpu.VMEM((rank, ratings.shape[0]), jnp.bfloat16),
            pltpu.VMEM(ratings.shape, jnp.bfloat16),
            pltpu.VMEM((rank, columns), jnp.float32),
            pltpu.SemaphoreType.DMA((2,)),
            pltpu.SemaphoreType.DMA((ratings.shape[0] // STRIPE,)),
        ],
        cost_estimate=pl.CostEstimate(flops=flops, bytes_accessed=4 * ratings.size, transcendentals=0),
        compiler_params=GRANT,
        name="residual",
    )(mask, counts, mine, other, item_blocks, ratings)


def user_share_body(item_ref, scaled_ref, mine_ref, other_ref):
    half = mine_ref.shape[0]
    item = item_ref[...]
    for start in range(0, scaled_ref.shape[0], STRIPE):
        stripe = pl.ds(start, STRIPE)
        share = lax.dot_general(
            item, scaled_ref[stripe], (((1,), (1,)), ((), ())), preferred_element_type=jnp.float32
        ).astype(jnp.bfloat16)
        mine_ref[:, stripe] = share[:half]
        other_ref[:, stripe] = share[half:]


def user_share_of(item, scaled):
    shape = jax.ShapeDtypeStruct((item.shape[0] // 2, scaled.shape[0]), jnp.bfloat16)
    return pl.pallas_call(
        user_share_body,
        in_specs=[VMEM, VMEM],
        out_specs=[VMEM, VMEM],
        out_shape=[shape, shape],
        cost_estimate=pl.CostEstimate(flops=2 * item.shape[0] * scaled.size, bytes_accessed=0, transcendentals=0),
        compiler_params=GRANT,
        name="user_share",
    )(item, scaled)


def halves_body(col_ref, mine_ref, arrived_ref, *block_refs):
    count = mine_ref.shape[0]
    for by, block_ref in enumerate(block_refs):
        at = lax.rem(col_ref[0] + by, count)
        block = mine_ref[at].astype(jnp.float32) + arrived_ref[at].astype(jnp.float32)
        block_ref[...] = block.astype(jnp.bfloat16)


def halves_summed(col, mine, arrived):
    count, *block = mine.shape
    shape = jax.ShapeDtypeStruct(tuple(block), jnp.bfloat16)
    return pl.pallas_call(
        halves_body,
        in_specs=[SMEM, VMEM, VMEM],
        out_specs=[VMEM] * count,
        out_shape=[shape] * count,
        compiler_params=GRANT,
        name="halves",
    )(col, mine, arrived)


def blocks_body(*refs):
    *block_refs, total_ref = refs
    total = block_refs[0][...].astype(jnp.float32)
    for block_ref in block_refs[1:]:
        total = total + block_ref[...].astype(jnp.float32)
    total_ref[...] = total.astype(jnp.bfloat16)


def blocks_summed(blocks):
    return pl.pallas_call(
        blocks_body,
        in_specs=[VMEM] * len(blocks),
        out_specs=VMEM,
        out_shape=jax.ShapeDtypeStruct(blocks[0].shape, jnp.bfloat16),
        compiler_params=GRANT,
        name="blocks",
    )(*blocks)


def summed(blocks_ref):
    total = blocks_ref[0].astype(jnp.float32)
    for i in range(1, blocks_ref.shape[0]):
        total = total + blocks_ref[i].astype(jnp.float32)
    return total


def item_raw_body(layer_ref, mask_ref, counts_ref, arrived_ref, user_ref, item_ref, error_ref, raw_ref, sums_ref):
    raw = summed(arrived_ref)
    raw_ref[...] = turned_by_core(raw, layer_ref[0])
    user, item = user_ref[...], item_ref[...]
    lane = lax.broadcasted_iota(jnp.int32, sums_ref.shape, 1)
    sums = jnp.zeros(sums_ref.shape, jnp.float32)
    for at, value in enumerate(
        (
            jnp.sum((mask_ref[...] * counts_ref[...]).astype(jnp.float32)),
            jnp.sum(user * user) + jnp.sum(item * item),
            jnp.sum(error_ref[...]),
            jnp.sum(raw * raw),
        )
    ):
        sums = jnp.where(lane == at, value, sums)
    sums_ref[...] = sums


def item_raw_of(layer, mask, counts, arrived, user_factor, item_factor, error):
    return pl.pallas_call(
        item_raw_body,
        in_specs=[SMEM] + [VMEM] * 6,
        out_specs=[VMEM, VMEM],
        out_shape=[
            jax.ShapeDtypeStruct(arrived.shape[1:], jnp.float32),
            jax.ShapeDtypeStruct((1, LANES), jnp.float32),
        ],
        compiler_params=GRANT,
        name="item_raw",
    )(layer, mask, counts, arrived, user_factor, item_factor, error)


def user_raw_body(arrived_ref, sums_ref, raw_ref, packed_ref):
    raw = summed(arrived_ref)
    raw_ref[...] = raw
    lane = lax.broadcasted_iota(jnp.int32, sums_ref.shape, 1)
    sums = sums_ref[...] + jnp.where(lane == 3, jnp.sum(raw * raw), 0.0)
    packed_ref[...] = jnp.broadcast_to(sums[None], packed_ref.shape)


def user_raw_of(arrived, sums, devices):
    return pl.pallas_call(
        user_raw_body,
        in_specs=[VMEM, VMEM],
        out_specs=[VMEM, VMEM],
        out_shape=[
            jax.ShapeDtypeStruct(arrived.shape[1:], jnp.float32),
            jax.ShapeDtypeStruct((devices, *sums.shape), jnp.float32),
        ],
        compiler_params=GRANT,
        name="user_raw",
    )(arrived, sums)


def packed_again_body(arrived_ref, packed_ref):
    packed_ref[...] = jnp.broadcast_to(summed(arrived_ref)[None], packed_ref.shape)


def packed_again(arrived, devices):
    return pl.pallas_call(
        packed_again_body,
        in_specs=[VMEM],
        out_specs=VMEM,
        out_shape=jax.ShapeDtypeStruct((devices, *arrived.shape[1:]), jnp.float32),
        compiler_params=GRANT,
        name="packed_again",
    )(arrived)


def step_body(arrived_ref, user_ref, item_ref, raw_user_ref, raw_item_ref, new_user_ref, new_item_ref, ends_ref):
    sums = summed(arrived_ref)
    lane = lax.broadcasted_iota(jnp.int32, sums.shape, 1)

    def lane_at(at):
        return jnp.sum(jnp.where(lane == at, sums, 0.0), axis=1, keepdims=True)

    observed_total = jnp.maximum(lane_at(0), 1.0)
    scale = 2.0 / observed_total
    grad_norm = scale * jnp.sqrt(lane_at(3) + epsilon)
    step_size = trust_ratio * jnp.sqrt(lane_at(1) + epsilon) / grad_norm * scale
    new_user_ref[...] = user_ref[...] - step_size * raw_user_ref[...]
    new_item_ref[...] = item_ref[...] - step_size * raw_item_ref[...]
    ends_ref[...] = jnp.where(lane == 0, lane_at(2) / observed_total, grad_norm)


def stepped(arrived, user_factor, item_factor, raw_user, raw_item):
    return pl.pallas_call(
        step_body,
        in_specs=[VMEM] * 5,
        out_specs=[VMEM] * 3,
        out_shape=[
            jax.ShapeDtypeStruct(user_factor.shape, jnp.float32),
            jax.ShapeDtypeStruct(item_factor.shape, jnp.float32),
            jax.ShapeDtypeStruct(arrived.shape[1:], jnp.float32),
        ],
        compiler_params=GRANT,
        name="step",
    )(arrived, user_factor, item_factor, raw_user, raw_item)


def exchanged(blocks, axis):
    return lax.all_to_all(blocks, axis, 0, 0, tiled=True)


def shifted(array, axis, by):
    count = lax.axis_size(axis)
    return lax.ppermute(array, axis, [(i, (i + by) % count) for i in range(count)])


def body(ratings, tile_mask, tile_counts, user_factor, item_factor):
    rows, width = lax.axis_size("row"), lax.axis_size("col_0")
    layer, col_0 = (lax.axis_index(axis).astype(jnp.int32)[None] for axis in ("layer", "col_0"))
    mask, counts = tile_mask.T, tile_counts.T
    user_low, item_blocks = lowered(layer, user_factor, item_factor, rows)
    item_blocks = exchanged(item_blocks, "row")
    mine = lax.all_gather(user_low, ("col_0", "col_1"), axis=0, tiled=True)
    other = shifted(mine, "layer", 1)
    scaled, item_share, item, error = residual_of(mask, counts, mine, other, item_blocks, ratings)
    item_arrived = exchanged(item_share, "row")
    my_share, other_share = user_share_of(item, scaled)
    partner_share = shifted(other_share, "layer", 1)
    blocked = (width, user_factor.shape[0] * width, user_factor.shape[1])
    blocks = halves_summed(col_0, my_share.reshape(blocked), partner_share.reshape(blocked))
    blocks = [blocks[0]] + [shifted(blocks[by], "col_0", by) for by in range(1, width)]
    quarter = blocks_summed(blocks)
    user_arrived = exchanged(quarter.reshape(width, *user_factor.shape), "col_1")
    raw_item, sums = item_raw_of(layer, mask, counts, item_arrived, user_factor, item_factor, error)
    raw_user, packed = user_raw_of(user_arrived, sums, lax.axis_size(COL_LAYER))
    packed = exchanged(packed, COL_LAYER)
    packed = packed_again(packed, rows)
    packed = exchanged(packed, "row")
    new_user, new_item, ends = stepped(packed, user_factor, item_factor, raw_user, raw_item)
    return (new_user, new_item, ends[0, 0], ends[0, 1])


def solution(mesh):
    finer = Mesh(
        mesh.devices.reshape(mesh.shape["row"], 4, 4, mesh.shape["layer"]),
        ("row", "col_0", "col_1", "layer"),
    )
    return jax.shard_map(
        body,
        mesh=finer,
        in_specs=(
            P("row", COL_LAYER),
            P("row", COL_LAYER),
            P("row", COL_LAYER),
            P(COL_LAYER, "row"),
            P("row", COL_LAYER),
        ),
        out_specs=(P(COL_LAYER, "row"), P("row", COL_LAYER), P(), P()),
        check_vma=False,
    )
```

```python
import jax
import jax.numpy as jnp
from jax import lax
from jax.experimental import pallas as pl
from jax.experimental.pallas import tpu as pltpu
from jax.sharding import Mesh
from jax.sharding import PartitionSpec as P

TILE = 128
LANES = 128
STRIPE = 512
COL_LAYER = ("col_0", "col_1", "layer")
VMEM = pl.BlockSpec(memory_space=pltpu.VMEM)
SMEM = pl.BlockSpec(memory_space=pltpu.SMEM)
FAR = pl.BlockSpec(memory_space=pltpu.HBM)
GRANT = pltpu.CompilerParams(vmem_limit_bytes=16 * 2**20)

epsilon = 1e-12
trust_ratio = 0.2


def lower_body(user_ref, blocks_ref):
    user = user_ref[...].astype(jnp.bfloat16)
    blocks_ref[...] = jnp.broadcast_to(user[None], blocks_ref.shape)


def lowered_for_all(factor, devices):
    return pl.pallas_call(
        lower_body,
        in_specs=[VMEM],
        out_specs=VMEM,
        out_shape=jax.ShapeDtypeStruct((devices, *factor.shape), jnp.bfloat16),
        compiler_params=GRANT,
        name="lower",
    )(factor)


def residual_body(
    far_mask_ref, far_counts_ref, far_user_ref, far_item_ref, far_ratings_ref,
    scaled_ref, item_share_ref, error_ref,
    mask_ref, counts_ref, user_ref, item_ref, ratings_ref, total_ref, sems, ratings_sems,
):
    columns = ratings_ref.shape[1]
    starts = range(0, ratings_ref.shape[0], STRIPE)
    stripes = [pl.ds(start, STRIPE) for start in starts]
    copies = [
        pltpu.make_async_copy(far, near, sems.at[at])
        for at, (far, near) in enumerate(
            (
                (far_user_ref, user_ref),
                (far_item_ref, item_ref),
                (far_mask_ref, mask_ref),
                (far_counts_ref, counts_ref),
            )
        )
    ]
    ratings_copies = [
        pltpu.make_async_copy(far_ratings_ref.at[stripe], ratings_ref.at[stripe], ratings_sems.at[at])
        for at, stripe in enumerate(stripes)
    ]
    for copy in copies + ratings_copies:
        copy.start()
    for copy in copies:
        copy.wait()
    item = item_ref[...]
    side = (TILE, TILE)
    position = lax.broadcasted_iota(jnp.int32, side, 0) * TILE + lax.broadcasted_iota(jnp.int32, side, 1)

    def predicted_of(at):
        user = user_ref[:, stripes[at]]
        return lax.dot_general(user, item, (((0,), (0,)), ((), ())), preferred_element_type=jnp.float32)

    def add_share(at):
        share = jnp.dot(user_ref[:, stripes[at]], scaled_ref[stripes[at]], preferred_element_type=jnp.float32)
        if at > 0:
            share = share + total_ref[...]
        if at + 1 < len(stripes):
            total_ref[...] = share
        else:
            item_share_ref[...] = share.astype(jnp.bfloat16).reshape(item_share_ref.shape)

    predicted = predicted_of(0)
    errors = [jnp.zeros((8, TILE), jnp.float32)] * (columns // TILE)
    for at, start in enumerate(starts):
        ratings_copies[at].wait()
        following = predicted_of(at + 1) if at + 1 < len(stripes) else None
        for row in range(0, STRIPE, TILE):
            for column in range(0, columns, TILE):
                tile_at = (column // TILE, (start + row) // TILE)
                limit = jnp.where(mask_ref[tile_at] == 1, counts_ref[tile_at], 0)
                rows, cols = pl.ds(start + row, TILE), pl.ds(column, TILE)
                rating = ratings_ref[rows, cols].astype(jnp.float32)
                difference = predicted[row : row + TILE, column : column + TILE] - rating
                residual = jnp.where(position < limit, difference, 0.0)
                scaled_ref[rows, cols] = residual.astype(jnp.bfloat16)
                error = (residual * residual).reshape(TILE // 8, 8, TILE).sum(axis=0)
                errors[column // TILE] = errors[column // TILE] + error
        if at > 0:
            add_share(at - 1)
        predicted = following
    add_share(len(stripes) - 1)
    error_ref[...] = jnp.concatenate(errors, axis=1)


def residual_of(mask, counts, user, item, ratings, devices):
    rank, columns = item.shape
    flops = 4 * rank * ratings.size
    return pl.pallas_call(
        residual_body,
        in_specs=[FAR] * 5,
        out_specs=[VMEM] * 3,
        out_shape=[
            jax.ShapeDtypeStruct(ratings.shape, jnp.bfloat16),
            jax.ShapeDtypeStruct((devices, rank // devices, columns), jnp.bfloat16),
            jax.ShapeDtypeStruct((8, columns), jnp.float32),
        ],
        scratch_shapes=[
            pltpu.SMEM(mask.shape, jnp.int32),
            pltpu.SMEM(counts.shape, jnp.int32),
            pltpu.VMEM(user.shape, jnp.bfloat16),
            pltpu.VMEM(item.shape, jnp.bfloat16),
            pltpu.VMEM(ratings.shape, jnp.bfloat16),
            pltpu.VMEM((rank, columns), jnp.float32),
            pltpu.SemaphoreType.DMA((4,)),
            pltpu.SemaphoreType.DMA((ratings.shape[0] // STRIPE,)),
        ],
        cost_estimate=pl.CostEstimate(flops=flops, bytes_accessed=4 * ratings.size, transcendentals=0),
        compiler_params=GRANT,
        name="residual",
    )(mask, counts, user, item, ratings)


def user_share_body(layer_ref, item_ref, scaled_ref, mine_ref, other_ref):
    chips, height, _ = mine_ref.shape
    item = item_ref[...]
    first = layer_ref[0] == 0
    for start in range(0, scaled_ref.shape[0], STRIPE):
        stripe = pl.ds(start, STRIPE)
        share = lax.dot_general(item, scaled_ref[stripe], (((1,), (1,)), ((), ())), preferred_element_type=jnp.float32)
        share = share.reshape(chips, 2, height, STRIPE)
        even, odd = share[:, 0], share[:, 1]
        mine_ref[:, :, stripe] = jnp.where(first, even, odd).astype(jnp.bfloat16)
        other_ref[:, :, stripe] = jnp.where(first, odd, even).astype(jnp.bfloat16)


def user_share_of(layer, item, scaled, height):
    shape = jax.ShapeDtypeStruct((item.shape[0] // height // 2, height, scaled.shape[0]), jnp.bfloat16)
    return pl.pallas_call(
        user_share_body,
        in_specs=[SMEM, VMEM, VMEM],
        out_specs=[VMEM, VMEM],
        out_shape=[shape, shape],
        cost_estimate=pl.CostEstimate(flops=2 * item.shape[0] * scaled.size, bytes_accessed=0, transcendentals=0),
        compiler_params=GRANT,
        name="user_share",
    )(layer, item, scaled)


def halves_body(mine_ref, arrived_ref, total_ref):
    total_ref[...] = (mine_ref[...].astype(jnp.float32) + arrived_ref[...].astype(jnp.float32)).astype(jnp.bfloat16)


def halves_summed(mine, arrived):
    return pl.pallas_call(
        halves_body,
        in_specs=[VMEM, VMEM],
        out_specs=VMEM,
        out_shape=jax.ShapeDtypeStruct(mine.shape, jnp.bfloat16),
        compiler_params=GRANT,
        name="halves",
    )(mine, arrived)


def summed(blocks_ref):
    total = blocks_ref[0].astype(jnp.float32)
    for i in range(1, blocks_ref.shape[0]):
        total = total + blocks_ref[i].astype(jnp.float32)
    return total


def item_raw_body(mask_ref, counts_ref, arrived_ref, user_ref, item_ref, error_ref, raw_ref, sums_ref):
    raw = summed(arrived_ref)
    raw_ref[...] = raw
    user, item = user_ref[...], item_ref[...]
    lane = lax.broadcasted_iota(jnp.int32, sums_ref.shape, 1)
    sums = jnp.zeros(sums_ref.shape, jnp.float32)
    for at, value in enumerate(
        (
            jnp.sum((mask_ref[...] * counts_ref[...]).astype(jnp.float32)),
            jnp.sum(user * user) + jnp.sum(item * item),
            jnp.sum(error_ref[...]),
            jnp.sum(raw * raw),
        )
    ):
        sums = jnp.where(lane == at, value, sums)
    sums_ref[...] = sums


def item_raw_of(mask, counts, arrived, user_factor, item_factor, error):
    return pl.pallas_call(
        item_raw_body,
        in_specs=[VMEM] * 6,
        out_specs=[VMEM, VMEM],
        out_shape=[
            jax.ShapeDtypeStruct(arrived.shape[1:], jnp.float32),
            jax.ShapeDtypeStruct((1, LANES), jnp.float32),
        ],
        compiler_params=GRANT,
        name="item_raw",
    )(mask, counts, arrived, user_factor, item_factor, error)


def user_raw_body(arrived_ref, sums_ref, raw_ref, packed_ref):
    raw = summed(arrived_ref)
    raw_ref[...] = raw
    lane = lax.broadcasted_iota(jnp.int32, sums_ref.shape, 1)
    sums = sums_ref[...] + jnp.where(lane == 3, jnp.sum(raw * raw), 0.0)
    packed_ref[...] = jnp.broadcast_to(sums[None], packed_ref.shape)


def user_raw_of(arrived, sums, devices):
    return pl.pallas_call(
        user_raw_body,
        in_specs=[VMEM, VMEM],
        out_specs=[VMEM, VMEM],
        out_shape=[
            jax.ShapeDtypeStruct(arrived.shape[1:], jnp.float32),
            jax.ShapeDtypeStruct((devices, *sums.shape), jnp.float32),
        ],
        compiler_params=GRANT,
        name="user_raw",
    )(arrived, sums)


def packed_again_body(arrived_ref, packed_ref):
    packed_ref[...] = jnp.broadcast_to(summed(arrived_ref)[None], packed_ref.shape)


def packed_again(arrived, devices):
    return pl.pallas_call(
        packed_again_body,
        in_specs=[VMEM],
        out_specs=VMEM,
        out_shape=jax.ShapeDtypeStruct((devices, *arrived.shape[1:]), jnp.float32),
        compiler_params=GRANT,
        name="packed_again",
    )(arrived)


def step_body(arrived_ref, user_ref, item_ref, raw_user_ref, raw_item_ref, new_user_ref, new_item_ref, ends_ref):
    sums = summed(arrived_ref)
    lane = lax.broadcasted_iota(jnp.int32, sums.shape, 1)

    def lane_at(at):
        return jnp.sum(jnp.where(lane == at, sums, 0.0), axis=1, keepdims=True)

    observed_total = jnp.maximum(lane_at(0), 1.0)
    scale = 2.0 / observed_total
    grad_norm = scale * jnp.sqrt(lane_at(3) + epsilon)
    step_size = trust_ratio * jnp.sqrt(lane_at(1) + epsilon) / grad_norm * scale
    new_user_ref[...] = user_ref[...] - step_size * raw_user_ref[...]
    new_item_ref[...] = item_ref[...] - step_size * raw_item_ref[...]
    ends_ref[...] = jnp.where(lane == 0, lane_at(2) / observed_total, grad_norm)


def stepped(arrived, user_factor, item_factor, raw_user, raw_item):
    return pl.pallas_call(
        step_body,
        in_specs=[VMEM] * 5,
        out_specs=[VMEM] * 3,
        out_shape=[
            jax.ShapeDtypeStruct(user_factor.shape, jnp.float32),
            jax.ShapeDtypeStruct(item_factor.shape, jnp.float32),
            jax.ShapeDtypeStruct(arrived.shape[1:], jnp.float32),
        ],
        compiler_params=GRANT,
        name="step",
    )(arrived, user_factor, item_factor, raw_user, raw_item)


def exchanged(blocks, axis):
    return lax.all_to_all(blocks, axis, 0, 0, tiled=True)


def shifted(array, axis, by):
    count = lax.axis_size(axis)
    return lax.ppermute(array, axis, [(i, (i + by) % count) for i in range(count)])


def body(ratings, tile_mask, tile_counts, user_factor, item_factor):
    rows, height = lax.axis_size("row"), user_factor.shape[0]
    layer = lax.axis_index("layer").astype(jnp.int32)[None]
    mask, counts = tile_mask.T, tile_counts.T
    user = exchanged(lowered_for_all(user_factor, lax.axis_size(COL_LAYER)), COL_LAYER)
    user = user.reshape(-1, user_factor.shape[1])
    item = lax.all_gather(item_factor.astype(jnp.bfloat16), "row", axis=0, tiled=True)
    scaled, item_share, error = residual_of(mask, counts, user, item, ratings, rows)
    item_arrived = exchanged(item_share, "row")
    my_share, other_share = user_share_of(layer, item, scaled, height)
    partner_share = shifted(other_share, "layer", 1)
    halves = halves_summed(my_share, partner_share)
    user_arrived = exchanged(halves, ("col_0", "col_1"))
    raw_item, sums = item_raw_of(mask, counts, item_arrived, user_factor, item_factor, error)
    raw_user, packed = user_raw_of(user_arrived, sums, lax.axis_size(COL_LAYER))
    packed = exchanged(packed, COL_LAYER)
    packed = packed_again(packed, rows)
    packed = exchanged(packed, "row")
    new_user, new_item, ends = stepped(packed, user_factor, item_factor, raw_user, raw_item)
    return (new_user, new_item, ends[0, 0], ends[0, 1])


def solution(mesh):
    finer = Mesh(
        mesh.devices.reshape(mesh.shape["row"], 4, 4, mesh.shape["layer"]),
        ("row", "col_0", "col_1", "layer"),
    )
    return jax.shard_map(
        body,
        mesh=finer,
        in_specs=(
            P("row", COL_LAYER),
            P("row", COL_LAYER),
            P("row", COL_LAYER),
            P(COL_LAYER, "row"),
            P("row", COL_LAYER),
        ),
        out_specs=(P(COL_LAYER, "row"), P("row", COL_LAYER), P(), P()),
        check_vma=False,
    )
```

```python
import jax
import jax.numpy as jnp
from jax import lax
from jax.experimental import pallas as pl
from jax.experimental.pallas import tpu as pltpu
from jax.sharding import Mesh
from jax.sharding import PartitionSpec as P

TILE = 128
LANES = 128
STRIPE = 512
GATHER_FIRST, SCATTER_FIRST = 0, 9
COL_LAYER = ("col_0", "col_1", "layer")
VMEM = pl.BlockSpec(memory_space=pltpu.VMEM)
SMEM = pl.BlockSpec(memory_space=pltpu.SMEM)
FAR = pl.BlockSpec(memory_space=pltpu.HBM)
GRANT = pltpu.CompilerParams(vmem_limit_bytes=16 * 2**20)
MOST_GRANT = pltpu.CompilerParams(vmem_limit_bytes=52 * 2**20)
WHOLE_GRANT = pltpu.CompilerParams(vmem_limit_bytes=60 * 2**20)

epsilon = 1e-12
trust_ratio = 0.2


def lower_body(user_ref, blocks_ref):
    user = user_ref[...].astype(jnp.bfloat16)
    blocks_ref[...] = jnp.broadcast_to(user[None], blocks_ref.shape)


def lowered_for_all(factor, devices):
    return pl.pallas_call(
        lower_body,
        in_specs=[VMEM],
        out_specs=VMEM,
        out_shape=jax.ShapeDtypeStruct((devices, *factor.shape), jnp.bfloat16),
        compiler_params=WHOLE_GRANT,
        name="lower",
    )(factor)


def residual_body(
    far_mask_ref, far_counts_ref, far_user_ref, far_item_ref, far_ratings_ref,
    scaled_ref, item_share_ref, error_ref,
    mask_ref, counts_ref, user_ref, item_ref, ratings_ref, total_ref, sems, ratings_sems,
):
    columns = ratings_ref.shape[1]
    starts = range(0, ratings_ref.shape[0], STRIPE)
    stripes = [pl.ds(start, STRIPE) for start in starts]
    rank = item_ref.shape[0]
    turn = GATHER_FIRST * rank // 16
    pairs = [(far_user_ref, user_ref), (far_mask_ref, mask_ref), (far_counts_ref, counts_ref)]
    pairs.append((far_item_ref.at[pl.ds(0, rank - turn)], item_ref.at[pl.ds(turn, rank - turn)]))
    if turn:
        pairs.append((far_item_ref.at[pl.ds(rank - turn, turn)], item_ref.at[pl.ds(0, turn)]))
    copies = [pltpu.make_async_copy(far, near, sems.at[at]) for at, (far, near) in enumerate(pairs)]
    ratings_copies = [
        pltpu.make_async_copy(far_ratings_ref.at[stripe], ratings_ref.at[stripe], ratings_sems.at[at])
        for at, stripe in enumerate(stripes)
    ]
    for copy in copies + ratings_copies:
        copy.start()
    for copy in copies:
        copy.wait()
    item = item_ref[...]
    side = (TILE, TILE)
    position = lax.broadcasted_iota(jnp.int32, side, 0) * TILE + lax.broadcasted_iota(jnp.int32, side, 1)

    def predicted_of(at):
        user = user_ref[:, stripes[at]]
        return lax.dot_general(user, item, (((0,), (0,)), ((), ())), preferred_element_type=jnp.float32)

    def add_share(at):
        share = jnp.dot(user_ref[:, stripes[at]], scaled_ref[stripes[at]], preferred_element_type=jnp.float32)
        if at > 0:
            share = share + total_ref[...]
        if at + 1 < len(stripes):
            total_ref[...] = share
        else:
            blocks = share.astype(jnp.bfloat16).reshape(item_share_ref.shape)
            first = SCATTER_FIRST * blocks.shape[0] // 16
            item_share_ref[...] = jnp.concatenate([blocks[first:], blocks[:first]]) if first else blocks

    predicted = predicted_of(0)
    errors = [jnp.zeros((8, TILE), jnp.float32)] * (columns // TILE)
    for at, start in enumerate(starts):
        ratings_copies[at].wait()
        following = predicted_of(at + 1) if at + 1 < len(stripes) else None
        for row in range(0, STRIPE, TILE):
            for column in range(0, columns, TILE):
                tile_at = (column // TILE, (start + row) // TILE)
                limit = jnp.where(mask_ref[tile_at] == 1, counts_ref[tile_at], 0)
                rows, cols = pl.ds(start + row, TILE), pl.ds(column, TILE)
                rating = ratings_ref[rows, cols].astype(jnp.float32)
                difference = predicted[row : row + TILE, column : column + TILE] - rating
                residual = jnp.where(position < limit, difference, 0.0)
                scaled_ref[rows, cols] = residual.astype(jnp.bfloat16)
                error = (residual * residual).reshape(TILE // 8, 8, TILE).sum(axis=0)
                errors[column // TILE] = errors[column // TILE] + error
        if at > 0:
            add_share(at - 1)
        predicted = following
    add_share(len(stripes) - 1)
    error_ref[...] = jnp.concatenate(errors, axis=1)


def residual_of(mask, counts, user, item, ratings, devices):
    rank, columns = item.shape
    flops = 4 * rank * ratings.size
    return pl.pallas_call(
        residual_body,
        in_specs=[FAR] * 5,
        out_specs=[VMEM] * 3,
        out_shape=[
            jax.ShapeDtypeStruct(ratings.shape, jnp.bfloat16),
            jax.ShapeDtypeStruct((devices, rank // devices, columns), jnp.bfloat16),
            jax.ShapeDtypeStruct((8, columns), jnp.float32),
        ],
        scratch_shapes=[
            pltpu.SMEM(mask.shape, jnp.int32),
            pltpu.SMEM(counts.shape, jnp.int32),
            pltpu.VMEM(user.shape, jnp.bfloat16),
            pltpu.VMEM(item.shape, jnp.bfloat16),
            pltpu.VMEM(ratings.shape, jnp.bfloat16),
            pltpu.VMEM((rank, columns), jnp.float32),
            pltpu.SemaphoreType.DMA((5,)),
            pltpu.SemaphoreType.DMA((ratings.shape[0] // STRIPE,)),
        ],
        cost_estimate=pl.CostEstimate(flops=flops, bytes_accessed=4 * ratings.size, transcendentals=0),
        compiler_params=MOST_GRANT,
        name="residual",
    )(mask, counts, user, item, ratings)


def user_share_body(layer_ref, item_ref, scaled_ref, mine_ref, other_ref):
    chips, height, _ = mine_ref.shape
    item = item_ref[...]
    first = layer_ref[0] == 0
    for start in range(0, scaled_ref.shape[0], STRIPE):
        stripe = pl.ds(start, STRIPE)
        share = lax.dot_general(item, scaled_ref[stripe], (((1,), (1,)), ((), ())), preferred_element_type=jnp.float32)
        share = share.reshape(chips, 2, height, STRIPE)
        for at in range(chips):
            even, odd = share[at, 0], share[at, 1]
            chip = (at + GATHER_FIRST * chips // 16) % chips
            mine_ref[chip, :, stripe] = jnp.where(first, even, odd).astype(jnp.bfloat16)
            other_ref[chip, :, stripe] = jnp.where(first, odd, even).astype(jnp.bfloat16)


def user_share_of(layer, item, scaled, height):
    shape = jax.ShapeDtypeStruct((item.shape[0] // height // 2, height, scaled.shape[0]), jnp.bfloat16)
    return pl.pallas_call(
        user_share_body,
        in_specs=[SMEM, VMEM, VMEM],
        out_specs=[VMEM, VMEM],
        out_shape=[shape, shape],
        cost_estimate=pl.CostEstimate(flops=2 * item.shape[0] * scaled.size, bytes_accessed=0, transcendentals=0),
        compiler_params=GRANT,
        name="user_share",
    )(layer, item, scaled)


def halves_body(mine_ref, arrived_ref, total_ref):
    total_ref[...] = (mine_ref[...].astype(jnp.float32) + arrived_ref[...].astype(jnp.float32)).astype(jnp.bfloat16)


def halves_summed(mine, arrived):
    return pl.pallas_call(
        halves_body,
        in_specs=[VMEM, VMEM],
        out_specs=VMEM,
        out_shape=jax.ShapeDtypeStruct(mine.shape, jnp.bfloat16),
        compiler_params=GRANT,
        name="halves",
    )(mine, arrived)


def summed(blocks_ref):
    total = blocks_ref[0].astype(jnp.float32)
    for i in range(1, blocks_ref.shape[0]):
        total = total + blocks_ref[i].astype(jnp.float32)
    return total


def item_raw_body(mask_ref, counts_ref, arrived_ref, user_ref, item_ref, error_ref, raw_ref, sums_ref):
    raw = summed(arrived_ref)
    raw_ref[...] = raw
    user, item = user_ref[...], item_ref[...]
    lane = lax.broadcasted_iota(jnp.int32, sums_ref.shape, 1)
    sums = jnp.zeros(sums_ref.shape, jnp.float32)
    for at, value in enumerate(
        (
            jnp.sum((mask_ref[...] * counts_ref[...]).astype(jnp.float32)),
            jnp.sum(user * user) + jnp.sum(item * item),
            jnp.sum(error_ref[...]),
            jnp.sum(raw * raw),
        )
    ):
        sums = jnp.where(lane == at, value, sums)
    sums_ref[...] = sums


def item_raw_of(mask, counts, arrived, user_factor, item_factor, error):
    return pl.pallas_call(
        item_raw_body,
        in_specs=[VMEM] * 6,
        out_specs=[VMEM, VMEM],
        out_shape=[
            jax.ShapeDtypeStruct(arrived.shape[1:], jnp.float32),
            jax.ShapeDtypeStruct((1, LANES), jnp.float32),
        ],
        compiler_params=GRANT,
        name="item_raw",
    )(mask, counts, arrived, user_factor, item_factor, error)


def user_raw_body(arrived_ref, sums_ref, raw_ref, packed_ref):
    raw = summed(arrived_ref)
    raw_ref[...] = raw
    lane = lax.broadcasted_iota(jnp.int32, sums_ref.shape, 1)
    sums = sums_ref[...] + jnp.where(lane == 3, jnp.sum(raw * raw), 0.0)
    packed_ref[...] = jnp.broadcast_to(sums[None], packed_ref.shape)


def user_raw_of(arrived, sums, devices):
    return pl.pallas_call(
        user_raw_body,
        in_specs=[VMEM, VMEM],
        out_specs=[VMEM, VMEM],
        out_shape=[
            jax.ShapeDtypeStruct(arrived.shape[1:], jnp.float32),
            jax.ShapeDtypeStruct((devices, *sums.shape), jnp.float32),
        ],
        compiler_params=GRANT,
        name="user_raw",
    )(arrived, sums)


def packed_again_body(arrived_ref, packed_ref):
    packed_ref[...] = jnp.broadcast_to(summed(arrived_ref)[None], packed_ref.shape)


def packed_again(arrived, devices):
    return pl.pallas_call(
        packed_again_body,
        in_specs=[VMEM],
        out_specs=VMEM,
        out_shape=jax.ShapeDtypeStruct((devices, *arrived.shape[1:]), jnp.float32),
        compiler_params=GRANT,
        name="packed_again",
    )(arrived)


def step_body(arrived_ref, user_ref, item_ref, raw_user_ref, raw_item_ref, new_user_ref, new_item_ref, loss_ref, norm_ref):
    sums = summed(arrived_ref)
    lane = lax.broadcasted_iota(jnp.int32, sums.shape, 1)

    def lane_at(at):
        return jnp.sum(jnp.where(lane == at, sums, 0.0), axis=1, keepdims=True)

    observed_total = jnp.maximum(lane_at(0), 1.0)
    scale = 2.0 / observed_total
    grad_norm = scale * jnp.sqrt(lane_at(3) + epsilon)
    step_size = trust_ratio * jnp.sqrt(lane_at(1) + epsilon) / grad_norm * scale
    new_user_ref[...] = user_ref[...] - step_size * raw_user_ref[...]
    new_item_ref[...] = item_ref[...] - step_size * raw_item_ref[...]
    loss_ref[0, 0] = jnp.sum(lane_at(2) / observed_total)
    norm_ref[0, 0] = jnp.sum(grad_norm)


def stepped(arrived, user_factor, item_factor, raw_user, raw_item):
    return pl.pallas_call(
        step_body,
        in_specs=[VMEM] * 5,
        out_specs=[VMEM, VMEM, SMEM, SMEM],
        out_shape=[
            jax.ShapeDtypeStruct(user_factor.shape, jnp.float32),
            jax.ShapeDtypeStruct(item_factor.shape, jnp.float32),
            jax.ShapeDtypeStruct((1, 1), jnp.float32),
            jax.ShapeDtypeStruct((1, 1), jnp.float32),
        ],
        compiler_params=GRANT,
        name="step",
    )(arrived, user_factor, item_factor, raw_user, raw_item)


def exchanged(blocks, axis, groups=None):
    return lax.all_to_all(blocks, axis, 0, 0, tiled=True, axis_index_groups=groups)


def listed_from(first, count):
    return [[(first + i) % count for i in range(count)]]


def shifted(array, axis, by):
    count = lax.axis_size(axis)
    return lax.ppermute(array, axis, [(i, (i + by) % count) for i in range(count)])


def body(ratings, tile_mask, tile_counts, user_factor, item_factor):
    rows, height = lax.axis_size("row"), user_factor.shape[0]
    gather_list, scatter_list = (listed_from(first * rows // 16, rows) for first in (GATHER_FIRST, SCATTER_FIRST))
    layer = lax.axis_index("layer").astype(jnp.int32)[None]
    mask, counts = tile_mask.T, tile_counts.T
    user = exchanged(lowered_for_all(user_factor, lax.axis_size(COL_LAYER)), COL_LAYER)
    user = user.reshape(-1, user_factor.shape[1])
    item = lax.all_gather(item_factor.astype(jnp.bfloat16), "row", axis=0, tiled=True, axis_index_groups=gather_list)
    scaled, item_share, error = residual_of(mask, counts, user, item, ratings, rows)
    item_arrived = exchanged(item_share, "row", scatter_list)
    my_share, other_share = user_share_of(layer, item, scaled, height)
    partner_share = shifted(other_share, "layer", 1)
    halves = halves_summed(my_share, partner_share)
    user_arrived = exchanged(halves, ("col_0", "col_1"))
    raw_item, sums = item_raw_of(mask, counts, item_arrived, user_factor, item_factor, error)
    raw_user, packed = user_raw_of(user_arrived, sums, lax.axis_size(COL_LAYER))
    packed = exchanged(packed, COL_LAYER)
    packed = packed_again(packed, rows)
    packed = exchanged(packed, "row", scatter_list)
    new_user, new_item, loss_value, grad_norm = stepped(packed, user_factor, item_factor, raw_user, raw_item)
    return (new_user, new_item, loss_value.reshape(()), grad_norm.reshape(()))


def solution(mesh):
    finer = Mesh(
        mesh.devices.reshape(mesh.shape["row"], 4, 4, mesh.shape["layer"]),
        ("row", "col_0", "col_1", "layer"),
    )
    return jax.shard_map(
        body,
        mesh=finer,
        in_specs=(
            P("row", COL_LAYER),
            P("row", COL_LAYER),
            P("row", COL_LAYER),
            P(COL_LAYER, "row"),
            P("row", COL_LAYER),
        ),
        out_specs=(P(COL_LAYER, "row"), P("row", COL_LAYER), P(), P()),
        check_vma=False,
    )
```

```python
import jax
import jax.numpy as jnp
from jax import lax
from jax.experimental import pallas as pl
from jax.experimental.pallas import tpu as pltpu
from jax.sharding import Mesh
from jax.sharding import PartitionSpec as P

TILE = 128
LANES = 128
STRIPE = 512
GATHER_FIRST, SCATTER_FIRST, SCALARS_FIRST = 9, 1, 9
COL_LAYER = ("col_0", "col_1", "layer")
VMEM = pl.BlockSpec(memory_space=pltpu.VMEM)
SMEM = pl.BlockSpec(memory_space=pltpu.SMEM)
FAR = pl.BlockSpec(memory_space=pltpu.HBM)
GRANT = pltpu.CompilerParams(vmem_limit_bytes=16 * 2**20)
MOST_GRANT = pltpu.CompilerParams(vmem_limit_bytes=50 * 2**20)
LOWER_GRANT = pltpu.CompilerParams(vmem_limit_bytes=60 * 2**20)

epsilon = 1e-12
trust_ratio = 0.2


def lower_body(user_ref, item_ref, mask_ref, counts_ref, user_low_ref, item_blocks_ref, limits_ref):
    item = item_ref[...].astype(jnp.bfloat16)
    item_blocks_ref[...] = jnp.broadcast_to(item[None], item_blocks_ref.shape)
    user_low_ref[...] = user_ref[...].astype(jnp.bfloat16)
    limits_ref[...] = jnp.where(mask_ref[...] == 1, counts_ref[...], 0)


def lowered(user_factor, item_factor, mask, counts, devices):
    return pl.pallas_call(
        lower_body,
        in_specs=[VMEM] * 4,
        out_specs=[VMEM] * 3,
        out_shape=[
            jax.ShapeDtypeStruct(user_factor.shape, jnp.bfloat16),
            jax.ShapeDtypeStruct((devices, *item_factor.shape), jnp.bfloat16),
            jax.ShapeDtypeStruct(mask.shape, jnp.int32),
        ],
        compiler_params=LOWER_GRANT,
        name="lower",
    )(user_factor, item_factor, mask, counts)


def residual_body(
    layer_ref, far_limits_ref, mine_ref, other_ref, far_item_ref, far_ratings_ref,
    scaled_ref, item_share_ref, error_ref,
    limits_ref, user_ref, item_ref, ratings_ref, total_ref, sems, ratings_sems,
):
    columns = ratings_ref.shape[1]
    starts = range(0, ratings_ref.shape[0], STRIPE)
    stripes = [pl.ds(start, STRIPE) for start in starts]
    rank = item_ref.shape[0]
    turn = GATHER_FIRST * rank // 16
    layer = layer_ref[0]
    pairs = [(mine_ref, user_ref.at[:, layer]), (other_ref, user_ref.at[:, 1 - layer])]
    pairs.append((far_limits_ref, limits_ref))
    pairs.append((far_item_ref.at[pl.ds(0, rank - turn)], item_ref.at[pl.ds(turn, rank - turn)]))
    if turn:
        pairs.append((far_item_ref.at[pl.ds(rank - turn, turn)], item_ref.at[pl.ds(0, turn)]))
    copies = [pltpu.make_async_copy(far, near, sems.at[at]) for at, (far, near) in enumerate(pairs)]
    ratings_copies = [
        pltpu.make_async_copy(far_ratings_ref.at[stripe], ratings_ref.at[stripe], ratings_sems.at[at])
        for at, stripe in enumerate(stripes)
    ]
    for copy in copies + ratings_copies:
        copy.start()
    for copy in copies:
        copy.wait()
    item = item_ref[...]
    side = (TILE, TILE)

    def user_of(at):
        return user_ref[:, :, :, stripes[at]].reshape(rank, STRIPE)

    position = lax.broadcasted_iota(jnp.int32, side, 0) * TILE + lax.broadcasted_iota(jnp.int32, side, 1)

    def predicted_of(at):
        return lax.dot_general(user_of(at), item, (((0,), (0,)), ((), ())), preferred_element_type=jnp.float32)

    def add_share(at):
        share = jnp.dot(user_of(at), scaled_ref[stripes[at]], preferred_element_type=jnp.float32)
        if at > 0:
            share = share + total_ref[...]
        if at + 1 < len(stripes):
            total_ref[...] = share
        else:
            blocks = share.astype(jnp.bfloat16).reshape(item_share_ref.shape)
            first = SCATTER_FIRST * blocks.shape[0] // 16
            item_share_ref[...] = jnp.concatenate([blocks[first:], blocks[:first]]) if first else blocks

    predicted = predicted_of(0)
    errors = [jnp.zeros((8, TILE), jnp.float32)] * (columns // TILE)
    for at, start in enumerate(starts):
        ratings_copies[at].wait()
        following = predicted_of(at + 1) if at + 1 < len(stripes) else None
        for row in range(0, STRIPE, TILE):
            for column in range(0, columns, TILE):
                limit = limits_ref[column // TILE, (start + row) // TILE]
                rows, cols = pl.ds(start + row, TILE), pl.ds(column, TILE)
                rating = ratings_ref[rows, cols].astype(jnp.float32)
                difference = predicted[row : row + TILE, column : column + TILE] - rating
                residual = jnp.where(position < limit, difference, 0.0)
                scaled_ref[rows, cols] = residual.astype(jnp.bfloat16)
                error = (residual * residual).reshape(TILE // 8, 8, TILE).sum(axis=0)
                errors[column // TILE] = errors[column // TILE] + error
        if at > 0:
            add_share(at - 1)
        predicted = following
    add_share(len(stripes) - 1)
    error_ref[...] = jnp.concatenate(errors, axis=1)


def residual_of(layer, limits, mine, other, item, ratings, devices):
    rank, columns = item.shape
    flops = 4 * rank * ratings.size
    return pl.pallas_call(
        residual_body,
        in_specs=[SMEM] + [FAR] * 5,
        out_specs=[VMEM] * 3,
        out_shape=[
            jax.ShapeDtypeStruct(ratings.shape, jnp.bfloat16),
            jax.ShapeDtypeStruct((devices, rank // devices, columns), jnp.bfloat16),
            jax.ShapeDtypeStruct((8, columns), jnp.float32),
        ],
        scratch_shapes=[
            pltpu.SMEM(limits.shape, jnp.int32),
            pltpu.VMEM((mine.shape[0], 2, *mine.shape[1:]), jnp.bfloat16),
            pltpu.VMEM(item.shape, jnp.bfloat16),
            pltpu.VMEM(ratings.shape, jnp.bfloat16),
            pltpu.VMEM((rank, columns), jnp.float32),
            pltpu.SemaphoreType.DMA((5,)),
            pltpu.SemaphoreType.DMA((ratings.shape[0] // STRIPE,)),
        ],
        cost_estimate=pl.CostEstimate(flops=flops, bytes_accessed=4 * ratings.size, transcendentals=0),
        compiler_params=MOST_GRANT,
        name="residual",
    )(layer, limits, mine, other, item, ratings)


def user_share_body(layer_ref, item_ref, far_scaled_ref, mine_ref, other_ref, scaled_ref, sems):
    chips, height, _ = mine_ref.shape
    stripes = [pl.ds(start, STRIPE) for start in range(0, scaled_ref.shape[0], STRIPE)]
    copies = [
        pltpu.make_async_copy(far_scaled_ref.at[stripe], scaled_ref.at[stripe], sems.at[at])
        for at, stripe in enumerate(stripes)
    ]
    for copy in copies:
        copy.start()
    item = item_ref[...]
    first = layer_ref[0] == 0
    for stripe, copy in zip(stripes, copies):
        copy.wait()
        share = lax.dot_general(item, scaled_ref[stripe], (((1,), (1,)), ((), ())), preferred_element_type=jnp.float32)
        share = share.reshape(chips, 2, height, STRIPE)
        for at in range(chips):
            even, odd = share[at, 0], share[at, 1]
            chip = (at + GATHER_FIRST * chips // 16) % chips
            mine_ref[chip, :, stripe] = jnp.where(first, even, odd).astype(jnp.bfloat16)
            other_ref[chip, :, stripe] = jnp.where(first, odd, even).astype(jnp.bfloat16)


def user_share_of(layer, item, scaled, height):
    shape = jax.ShapeDtypeStruct((item.shape[0] // height // 2, height, scaled.shape[0]), jnp.bfloat16)
    return pl.pallas_call(
        user_share_body,
        in_specs=[SMEM, VMEM, FAR],
        out_specs=[VMEM, VMEM],
        out_shape=[shape, shape],
        scratch_shapes=[
            pltpu.VMEM(scaled.shape, jnp.bfloat16),
            pltpu.SemaphoreType.DMA((scaled.shape[0] // STRIPE,)),
        ],
        cost_estimate=pl.CostEstimate(flops=2 * item.shape[0] * scaled.size, bytes_accessed=0, transcendentals=0),
        compiler_params=MOST_GRANT,
        name="user_share",
    )(layer, item, scaled)


def halves_body(mine_ref, arrived_ref, total_ref):
    total_ref[...] = (mine_ref[...].astype(jnp.float32) + arrived_ref[...].astype(jnp.float32)).astype(jnp.bfloat16)


def halves_summed(mine, arrived):
    return pl.pallas_call(
        halves_body,
        in_specs=[VMEM, VMEM],
        out_specs=VMEM,
        out_shape=jax.ShapeDtypeStruct(mine.shape, jnp.bfloat16),
        compiler_params=GRANT,
        name="halves",
    )(mine, arrived)


def summed(blocks_ref):
    total = blocks_ref[0].astype(jnp.float32)
    for i in range(1, blocks_ref.shape[0]):
        total = total + blocks_ref[i].astype(jnp.float32)
    return total


def item_raw_body(limits_ref, arrived_ref, user_ref, item_ref, error_ref, raw_ref, sums_ref):
    raw = summed(arrived_ref)
    raw_ref[...] = raw
    user, item = user_ref[...], item_ref[...]
    lane = lax.broadcasted_iota(jnp.int32, sums_ref.shape, 1)
    sums = jnp.zeros(sums_ref.shape, jnp.float32)
    for at, value in enumerate(
        (
            jnp.sum(limits_ref[...].astype(jnp.float32)),
            jnp.sum(user * user) + jnp.sum(item * item),
            jnp.sum(error_ref[...]),
            jnp.sum(raw * raw),
        )
    ):
        sums = jnp.where(lane == at, value, sums)
    sums_ref[...] = sums


def item_raw_of(limits, arrived, user_factor, item_factor, error):
    return pl.pallas_call(
        item_raw_body,
        in_specs=[VMEM] * 5,
        out_specs=[VMEM, VMEM],
        out_shape=[
            jax.ShapeDtypeStruct(arrived.shape[1:], jnp.float32),
            jax.ShapeDtypeStruct((1, LANES), jnp.float32),
        ],
        compiler_params=GRANT,
        name="item_raw",
    )(limits, arrived, user_factor, item_factor, error)


def user_raw_body(arrived_ref, sums_ref, raw_ref, packed_ref):
    raw = summed(arrived_ref)
    raw_ref[...] = raw
    lane = lax.broadcasted_iota(jnp.int32, sums_ref.shape, 1)
    sums = sums_ref[...] + jnp.where(lane == 3, jnp.sum(raw * raw), 0.0)
    packed_ref[...] = jnp.broadcast_to(sums[None], packed_ref.shape)


def user_raw_of(arrived, sums, devices):
    return pl.pallas_call(
        user_raw_body,
        in_specs=[VMEM, VMEM],
        out_specs=[VMEM, VMEM],
        out_shape=[
            jax.ShapeDtypeStruct(arrived.shape[1:], jnp.float32),
            jax.ShapeDtypeStruct((devices, *sums.shape), jnp.float32),
        ],
        compiler_params=GRANT,
        name="user_raw",
    )(arrived, sums)


def packed_again_body(arrived_ref, packed_ref):
    packed_ref[...] = jnp.broadcast_to(summed(arrived_ref)[None], packed_ref.shape)


def packed_again(arrived, devices):
    return pl.pallas_call(
        packed_again_body,
        in_specs=[VMEM],
        out_specs=VMEM,
        out_shape=jax.ShapeDtypeStruct((devices, *arrived.shape[1:]), jnp.float32),
        compiler_params=GRANT,
        name="packed_again",
    )(arrived)


def step_body(arrived_ref, user_ref, item_ref, raw_user_ref, raw_item_ref, new_user_ref, new_item_ref, loss_ref, norm_ref):
    sums = summed(arrived_ref)
    lane = lax.broadcasted_iota(jnp.int32, sums.shape, 1)

    def lane_at(at):
        return jnp.sum(jnp.where(lane == at, sums, 0.0), axis=1, keepdims=True)

    observed_total = jnp.maximum(lane_at(0), 1.0)
    scale = 2.0 / observed_total
    grad_norm = scale * jnp.sqrt(lane_at(3) + epsilon)
    step_size = trust_ratio * jnp.sqrt(lane_at(1) + epsilon) / grad_norm * scale
    new_user_ref[...] = user_ref[...] - step_size * raw_user_ref[...]
    new_item_ref[...] = item_ref[...] - step_size * raw_item_ref[...]
    loss_ref[0, 0] = jnp.sum(lane_at(2) / observed_total)
    norm_ref[0, 0] = jnp.sum(grad_norm)


def stepped(arrived, user_factor, item_factor, raw_user, raw_item):
    return pl.pallas_call(
        step_body,
        in_specs=[VMEM] * 5,
        out_specs=[VMEM, VMEM, SMEM, SMEM],
        out_shape=[
            jax.ShapeDtypeStruct(user_factor.shape, jnp.float32),
            jax.ShapeDtypeStruct(item_factor.shape, jnp.float32),
            jax.ShapeDtypeStruct((1, 1), jnp.float32),
            jax.ShapeDtypeStruct((1, 1), jnp.float32),
        ],
        compiler_params=GRANT,
        name="step",
    )(arrived, user_factor, item_factor, raw_user, raw_item)


def exchanged(blocks, axis, groups=None):
    return lax.all_to_all(blocks, axis, 0, 0, tiled=True, axis_index_groups=groups)


def listed_from(first, count):
    return [[(first + i) % count for i in range(count)]]


def shifted(array, axis, by):
    count = lax.axis_size(axis)
    return lax.ppermute(array, axis, [(i, (i + by) % count) for i in range(count)])


def body(ratings, tile_mask, tile_counts, user_factor, item_factor):
    rows, height = lax.axis_size("row"), user_factor.shape[0]
    gather_list, scatter_list, scalars_list = (
        listed_from(first * rows // 16, rows) for first in (GATHER_FIRST, SCATTER_FIRST, SCALARS_FIRST)
    )
    layer = lax.axis_index("layer").astype(jnp.int32)[None]
    mask, counts = tile_mask.T, tile_counts.T
    user_low, item_blocks, limits = lowered(user_factor, item_factor, mask, counts, rows)
    item = exchanged(item_blocks, "row", gather_list).reshape(-1, item_factor.shape[1])
    mine = lax.all_gather(user_low, ("col_0", "col_1"), axis=0, tiled=True)
    mine = mine.reshape(-1, *user_factor.shape)
    other = shifted(mine, "layer", 1)
    scaled, item_share, error = residual_of(layer, limits, mine, other, item, ratings, rows)
    item_arrived = exchanged(item_share, "row", scatter_list)
    my_share, other_share = user_share_of(layer, item, scaled, height)
    partner_share = shifted(other_share, "layer", 1)
    halves = halves_summed(my_share, partner_share)
    user_arrived = exchanged(halves, ("col_0", "col_1"))
    raw_item, sums = item_raw_of(limits, item_arrived, user_factor, item_factor, error)
    raw_user, packed = user_raw_of(user_arrived, sums, lax.axis_size(COL_LAYER))
    packed = exchanged(packed, COL_LAYER)
    packed = packed_again(packed, rows)
    packed = exchanged(packed, "row", scalars_list)
    new_user, new_item, loss_value, grad_norm = stepped(packed, user_factor, item_factor, raw_user, raw_item)
    return (new_user, new_item, loss_value.reshape(()), grad_norm.reshape(()))


def solution(mesh):
    finer = Mesh(
        mesh.devices.reshape(mesh.shape["row"], 4, 4, mesh.shape["layer"]),
        ("row", "col_0", "col_1", "layer"),
    )
    return jax.shard_map(
        body,
        mesh=finer,
        in_specs=(
            P("row", COL_LAYER),
            P("row", COL_LAYER),
            P("row", COL_LAYER),
            P(COL_LAYER, "row"),
            P("row", COL_LAYER),
        ),
        out_specs=(P(COL_LAYER, "row"), P("row", COL_LAYER), P(), P()),
        check_vma=False,
    )
```

```python
import jax
import jax.numpy as jnp
from jax import lax
from jax.experimental import pallas as pl
from jax.experimental.pallas import tpu as pltpu
from jax.sharding import Mesh
from jax.sharding import PartitionSpec as P

TILE = 128
LANES = 128
STRIPE = 512
GATHER_FIRST, SCATTER_FIRST, SCALARS_FIRST, CHIP_FIRST = 9, 9, 8, 15
COL_LAYER = ("col_0", "col_1", "layer")
VMEM = pl.BlockSpec(memory_space=pltpu.VMEM)
SMEM = pl.BlockSpec(memory_space=pltpu.SMEM)
FAR = pl.BlockSpec(memory_space=pltpu.HBM)
GRANT = pltpu.CompilerParams(vmem_limit_bytes=16 * 2**20)
MOST_GRANT = pltpu.CompilerParams(vmem_limit_bytes=50 * 2**20)
WHOLE_GRANT = pltpu.CompilerParams(vmem_limit_bytes=60 * 2**20)

epsilon = 1e-12
trust_ratio = 0.2


def lower_body(user_ref, item_ref, mask_ref, counts_ref, user_blocks_ref, item_blocks_ref, limits_ref):
    user_blocks_ref[...] = jnp.broadcast_to(user_ref[...].astype(jnp.bfloat16)[None], user_blocks_ref.shape)
    item_blocks_ref[...] = jnp.broadcast_to(item_ref[...].astype(jnp.bfloat16)[None], item_blocks_ref.shape)
    limits_ref[...] = jnp.where(mask_ref[...] == 1, counts_ref[...], 0)


def lowered(user_factor, item_factor, mask, counts, chips, rows):
    return pl.pallas_call(
        lower_body,
        in_specs=[VMEM] * 4,
        out_specs=[VMEM] * 3,
        out_shape=[
            jax.ShapeDtypeStruct((chips, *user_factor.shape), jnp.bfloat16),
            jax.ShapeDtypeStruct((rows, *item_factor.shape), jnp.bfloat16),
            jax.ShapeDtypeStruct(mask.shape, jnp.int32),
        ],
        compiler_params=WHOLE_GRANT,
        name="lower",
    )(user_factor, item_factor, mask, counts)


def residual_body(
    layer_ref, far_limits_ref, mine_ref, other_ref, far_item_ref, far_ratings_ref,
    scaled_ref, item_share_ref, error_ref,
    limits_ref, user_ref, item_ref, ratings_ref, total_ref, sems, ratings_sems,
):
    columns = ratings_ref.shape[1]
    starts = range(0, ratings_ref.shape[0], STRIPE)
    stripes = [pl.ds(start, STRIPE) for start in starts]
    layer, chips, (rank, _) = layer_ref[0], mine_ref.shape[0], item_ref.shape
    turn = GATHER_FIRST * rank // 16
    pairs = [
        (far_limits_ref, limits_ref),
        (far_item_ref.at[pl.ds(0, rank - turn)], item_ref.at[pl.ds(turn, rank - turn)]),
        (far_item_ref.at[pl.ds(rank - turn, turn)], item_ref.at[pl.ds(0, turn)]),
    ]
    turn = CHIP_FIRST * chips // 16
    for half_ref, core in ((mine_ref, layer), (other_ref, 1 - layer)):
        pairs += [
            (half_ref.at[pl.ds(0, chips - turn)], user_ref.at[pl.ds(turn, chips - turn), core]),
            (half_ref.at[pl.ds(chips - turn, turn)], user_ref.at[pl.ds(0, turn), core]),
        ]
    copies = [pltpu.make_async_copy(far, near, sems.at[at]) for at, (far, near) in enumerate(pairs)]
    ratings_copies = [
        pltpu.make_async_copy(far_ratings_ref.at[stripe], ratings_ref.at[stripe], ratings_sems.at[at])
        for at, stripe in enumerate(stripes)
    ]
    for copy in copies + ratings_copies:
        copy.start()
    for copy in copies:
        copy.wait()
    item = item_ref[...]
    side = (TILE, TILE)

    def user_of(at):
        return user_ref[:, :, :, stripes[at]].reshape(rank, STRIPE)

    position = lax.broadcasted_iota(jnp.int32, side, 0) * TILE + lax.broadcasted_iota(jnp.int32, side, 1)

    def predicted_of(at):
        return lax.dot_general(user_of(at), item, (((0,), (0,)), ((), ())), preferred_element_type=jnp.float32)

    def add_share(at):
        share = jnp.dot(user_of(at), scaled_ref[stripes[at]], preferred_element_type=jnp.float32)
        if at > 0:
            share = share + total_ref[...]
        if at + 1 < len(stripes):
            total_ref[...] = share
        else:
            blocks = share.astype(jnp.bfloat16).reshape(item_share_ref.shape)
            first = SCATTER_FIRST * blocks.shape[0] // 16
            item_share_ref[...] = jnp.concatenate([blocks[first:], blocks[:first]]) if first else blocks

    predicted = predicted_of(0)
    errors = [jnp.zeros((8, TILE), jnp.float32)] * (columns // TILE)
    for at, start in enumerate(starts):
        ratings_copies[at].wait()
        following = predicted_of(at + 1) if at + 1 < len(stripes) else None
        for row in range(0, STRIPE, TILE):
            for column in range(0, columns, TILE):
                limit = limits_ref[column // TILE, (start + row) // TILE]
                rows, cols = pl.ds(start + row, TILE), pl.ds(column, TILE)
                rating = ratings_ref[rows, cols].astype(jnp.float32)
                difference = predicted[row : row + TILE, column : column + TILE] - rating
                residual = jnp.where(position < limit, difference, 0.0)
                scaled_ref[rows, cols] = residual.astype(jnp.bfloat16)
                error = (residual * residual).reshape(TILE // 8, 8, TILE).sum(axis=0)
                errors[column // TILE] = errors[column // TILE] + error
        if at > 0:
            add_share(at - 1)
        predicted = following
    add_share(len(stripes) - 1)
    error_ref[...] = jnp.concatenate(errors, axis=1)


def residual_of(layer, limits, mine, other, item, ratings, devices):
    rank, columns = item.shape
    flops = 4 * rank * ratings.size
    return pl.pallas_call(
        residual_body,
        in_specs=[SMEM] + [FAR] * 5,
        out_specs=[VMEM] * 3,
        out_shape=[
            jax.ShapeDtypeStruct(ratings.shape, jnp.bfloat16),
            jax.ShapeDtypeStruct((devices, rank // devices, columns), jnp.bfloat16),
            jax.ShapeDtypeStruct((8, columns), jnp.float32),
        ],
        scratch_shapes=[
            pltpu.SMEM(limits.shape, jnp.int32),
            pltpu.VMEM((mine.shape[0], 2, *mine.shape[1:]), jnp.bfloat16),
            pltpu.VMEM(item.shape, jnp.bfloat16),
            pltpu.VMEM(ratings.shape, jnp.bfloat16),
            pltpu.VMEM((rank, columns), jnp.float32),
            pltpu.SemaphoreType.DMA((7,)),
            pltpu.SemaphoreType.DMA((ratings.shape[0] // STRIPE,)),
        ],
        cost_estimate=pl.CostEstimate(flops=flops, bytes_accessed=4 * ratings.size, transcendentals=0),
        compiler_params=MOST_GRANT,
        name="residual",
    )(layer, limits, mine, other, item, ratings)


def user_share_body(layer_ref, item_ref, scaled_ref, mine_ref, other_ref):
    chips, height, _ = mine_ref.shape
    item = item_ref[...]
    first = layer_ref[0] == 0
    for start in range(0, scaled_ref.shape[0], STRIPE):
        stripe = pl.ds(start, STRIPE)
        share = lax.dot_general(item, scaled_ref[stripe], (((1,), (1,)), ((), ())), preferred_element_type=jnp.float32)
        share = share.reshape(chips, 2, height, STRIPE)
        for at in range(chips):
            even, odd = share[at, 0], share[at, 1]
            chip = (at + (GATHER_FIRST - CHIP_FIRST) * chips // 16) % chips
            mine_ref[chip, :, stripe] = jnp.where(first, even, odd).astype(jnp.bfloat16)
            other_ref[chip, :, stripe] = jnp.where(first, odd, even).astype(jnp.bfloat16)


def user_share_of(layer, item, scaled, height):
    shape = jax.ShapeDtypeStruct((item.shape[0] // height // 2, height, scaled.shape[0]), jnp.bfloat16)
    return pl.pallas_call(
        user_share_body,
        in_specs=[SMEM, VMEM, VMEM],
        out_specs=[VMEM, VMEM],
        out_shape=[shape, shape],
        cost_estimate=pl.CostEstimate(flops=2 * item.shape[0] * scaled.size, bytes_accessed=0, transcendentals=0),
        compiler_params=GRANT,
        name="user_share",
    )(layer, item, scaled)


def halves_body(mine_ref, arrived_ref, total_ref):
    total_ref[...] = (mine_ref[...].astype(jnp.float32) + arrived_ref[...].astype(jnp.float32)).astype(jnp.bfloat16)


def halves_summed(mine, arrived):
    return pl.pallas_call(
        halves_body,
        in_specs=[VMEM, VMEM],
        out_specs=VMEM,
        out_shape=jax.ShapeDtypeStruct(mine.shape, jnp.bfloat16),
        compiler_params=GRANT,
        name="halves",
    )(mine, arrived)


def summed(blocks_ref):
    total = blocks_ref[0].astype(jnp.float32)
    for i in range(1, blocks_ref.shape[0]):
        total = total + blocks_ref[i].astype(jnp.float32)
    return total


def item_raw_body(limits_ref, arrived_ref, user_ref, item_ref, error_ref, raw_ref, sums_ref):
    raw = summed(arrived_ref)
    raw_ref[...] = raw
    user, item = user_ref[...], item_ref[...]
    lane = lax.broadcasted_iota(jnp.int32, sums_ref.shape, 1)
    sums = jnp.zeros(sums_ref.shape, jnp.float32)
    for at, value in enumerate(
        (
            jnp.sum(limits_ref[...].astype(jnp.float32)),
            jnp.sum(user * user) + jnp.sum(item * item),
            jnp.sum(error_ref[...]),
            jnp.sum(raw * raw),
        )
    ):
        sums = jnp.where(lane == at, value, sums)
    sums_ref[...] = sums


def item_raw_of(limits, arrived, user_factor, item_factor, error):
    return pl.pallas_call(
        item_raw_body,
        in_specs=[VMEM] * 5,
        out_specs=[VMEM, VMEM],
        out_shape=[
            jax.ShapeDtypeStruct(arrived.shape[1:], jnp.float32),
            jax.ShapeDtypeStruct((1, LANES), jnp.float32),
        ],
        compiler_params=GRANT,
        name="item_raw",
    )(limits, arrived, user_factor, item_factor, error)


def user_raw_body(arrived_ref, sums_ref, raw_ref, packed_ref):
    raw = summed(arrived_ref)
    raw_ref[...] = raw
    lane = lax.broadcasted_iota(jnp.int32, sums_ref.shape, 1)
    sums = sums_ref[...] + jnp.where(lane == 3, jnp.sum(raw * raw), 0.0)
    packed_ref[...] = jnp.broadcast_to(sums[None], packed_ref.shape)


def user_raw_of(arrived, sums, devices):
    return pl.pallas_call(
        user_raw_body,
        in_specs=[VMEM, VMEM],
        out_specs=[VMEM, VMEM],
        out_shape=[
            jax.ShapeDtypeStruct(arrived.shape[1:], jnp.float32),
            jax.ShapeDtypeStruct((devices, *sums.shape), jnp.float32),
        ],
        compiler_params=GRANT,
        name="user_raw",
    )(arrived, sums)


def packed_again_body(arrived_ref, packed_ref):
    packed_ref[...] = jnp.broadcast_to(summed(arrived_ref)[None], packed_ref.shape)


def packed_again(arrived, devices):
    return pl.pallas_call(
        packed_again_body,
        in_specs=[VMEM],
        out_specs=VMEM,
        out_shape=jax.ShapeDtypeStruct((devices, *arrived.shape[1:]), jnp.float32),
        compiler_params=GRANT,
        name="packed_again",
    )(arrived)


def step_body(arrived_ref, user_ref, item_ref, raw_user_ref, raw_item_ref, new_user_ref, new_item_ref, loss_ref, norm_ref):
    sums = summed(arrived_ref)
    lane = lax.broadcasted_iota(jnp.int32, sums.shape, 1)

    def lane_at(at):
        return jnp.sum(jnp.where(lane == at, sums, 0.0), axis=1, keepdims=True)

    observed_total = jnp.maximum(lane_at(0), 1.0)
    scale = 2.0 / observed_total
    grad_norm = scale * jnp.sqrt(lane_at(3) + epsilon)
    step_size = trust_ratio * jnp.sqrt(lane_at(1) + epsilon) / grad_norm * scale
    new_user_ref[...] = user_ref[...] - step_size * raw_user_ref[...]
    new_item_ref[...] = item_ref[...] - step_size * raw_item_ref[...]
    loss_ref[0, 0] = jnp.sum(lane_at(2) / observed_total)
    norm_ref[0, 0] = jnp.sum(grad_norm)


def stepped(arrived, user_factor, item_factor, raw_user, raw_item):
    return pl.pallas_call(
        step_body,
        in_specs=[VMEM] * 5,
        out_specs=[VMEM, VMEM, SMEM, SMEM],
        out_shape=[
            jax.ShapeDtypeStruct(user_factor.shape, jnp.float32),
            jax.ShapeDtypeStruct(item_factor.shape, jnp.float32),
            jax.ShapeDtypeStruct((1, 1), jnp.float32),
            jax.ShapeDtypeStruct((1, 1), jnp.float32),
        ],
        compiler_params=GRANT,
        name="step",
    )(arrived, user_factor, item_factor, raw_user, raw_item)


def exchanged(blocks, axis, groups=None):
    return lax.all_to_all(blocks, axis, 0, 0, tiled=True, axis_index_groups=groups)


def listed_from(first, count):
    return [[(first + i) % count for i in range(count)]]


def shifted(array, axis, by):
    count = lax.axis_size(axis)
    return lax.ppermute(array, axis, [(i, (i + by) % count) for i in range(count)])


def body(ratings, tile_mask, tile_counts, user_factor, item_factor):
    rows, height = lax.axis_size("row"), user_factor.shape[0]
    devices, chips = lax.axis_size(COL_LAYER), lax.axis_size(("col_0", "col_1"))
    gather_list, scatter_list, scalars_list = (
        listed_from(first * rows // 16, rows) for first in (GATHER_FIRST, SCATTER_FIRST, SCALARS_FIRST)
    )
    chips_list, devices_list = (listed_from(CHIP_FIRST * count // 16, count) for count in (chips, devices))
    layer = lax.axis_index("layer").astype(jnp.int32)[None]
    user_blocks, item_blocks, limits = lowered(
        user_factor, item_factor, tile_mask.T, tile_counts.T, chips, rows
    )
    mine = exchanged(user_blocks, ("col_0", "col_1"), chips_list)
    item = exchanged(item_blocks, "row", gather_list).reshape(-1, item_factor.shape[1])
    other = shifted(mine, "layer", 1)
    scaled, item_share, error = residual_of(layer, limits, mine, other, item, ratings, rows)
    item_arrived = exchanged(item_share, "row", scatter_list)
    my_share, other_share = user_share_of(layer, item, scaled, height)
    partner_share = shifted(other_share, "layer", 1)
    halves = halves_summed(my_share, partner_share)
    user_arrived = exchanged(halves, ("col_0", "col_1"), chips_list)
    raw_item, sums = item_raw_of(limits, item_arrived, user_factor, item_factor, error)
    raw_user, packed = user_raw_of(user_arrived, sums, devices)
    packed = exchanged(packed, COL_LAYER, devices_list)
    packed = packed_again(packed, rows)
    packed = exchanged(packed, "row", scalars_list)
    new_user, new_item, loss_value, grad_norm = stepped(packed, user_factor, item_factor, raw_user, raw_item)
    return (new_user, new_item, loss_value.reshape(()), grad_norm.reshape(()))


def solution(mesh):
    finer = Mesh(
        mesh.devices.reshape(mesh.shape["row"], 4, 4, mesh.shape["layer"]),
        ("row", "col_0", "col_1", "layer"),
    )
    return jax.shard_map(
        body,
        mesh=finer,
        in_specs=(
            P("row", COL_LAYER),
            P("row", COL_LAYER),
            P("row", COL_LAYER),
            P(COL_LAYER, "row"),
            P("row", COL_LAYER),
        ),
        out_specs=(P(COL_LAYER, "row"), P("row", COL_LAYER), P(), P()),
        check_vma=False,
    )
```

```python
import jax
import jax.numpy as jnp
from jax import lax
from jax.experimental import pallas as pl
from jax.experimental.pallas import tpu as pltpu
from jax.sharding import Mesh
from jax.sharding import PartitionSpec as P

TILE = 128
LANES = 128
STRIPE = 512
SCATTER_FIRST, SCALARS_FIRST, CHIP_FIRST = 9, 8, 15
COL_LAYER = ("col_0", "col_1", "layer")
VMEM = pl.BlockSpec(memory_space=pltpu.VMEM)
SMEM = pl.BlockSpec(memory_space=pltpu.SMEM)
FAR = pl.BlockSpec(memory_space=pltpu.HBM)
GRANT = pltpu.CompilerParams(vmem_limit_bytes=16 * 2**20)
MOST_GRANT = pltpu.CompilerParams(vmem_limit_bytes=50 * 2**20)
WHOLE_GRANT = pltpu.CompilerParams(vmem_limit_bytes=60 * 2**20)

epsilon = 1e-12
trust_ratio = 0.2


def lower_body(user_ref, mask_ref, counts_ref, blocks_ref, limits_ref):
    user = user_ref[...].astype(jnp.bfloat16)
    blocks_ref[...] = jnp.broadcast_to(user[None], blocks_ref.shape)
    limits_ref[...] = jnp.where(mask_ref[...] == 1, counts_ref[...], 0)


def lowered_for_all(factor, mask, counts, devices):
    return pl.pallas_call(
        lower_body,
        in_specs=[VMEM] * 3,
        out_specs=[VMEM] * 2,
        out_shape=[
            jax.ShapeDtypeStruct((devices, *factor.shape), jnp.bfloat16),
            jax.ShapeDtypeStruct(mask.shape, jnp.int32),
        ],
        compiler_params=WHOLE_GRANT,
        name="lower",
    )(factor, mask, counts)


def residual_body(
    far_limits_ref, far_user_ref, far_item_ref, far_ratings_ref,
    scaled_ref, item_share_ref, error_ref,
    limits_ref, user_ref, item_ref, ratings_ref, total_ref, sems, ratings_sems,
):
    columns = ratings_ref.shape[1]
    starts = range(0, ratings_ref.shape[0], STRIPE)
    stripes = [pl.ds(start, STRIPE) for start in starts]
    rank = user_ref.shape[0]
    turn = CHIP_FIRST * rank // 16
    pairs = [
        (far_item_ref, item_ref),
        (far_limits_ref, limits_ref),
        (far_user_ref.at[pl.ds(0, rank - turn)], user_ref.at[pl.ds(turn, rank - turn)]),
        (far_user_ref.at[pl.ds(rank - turn, turn)], user_ref.at[pl.ds(0, turn)]),
    ]
    copies = [pltpu.make_async_copy(far, near, sems.at[at]) for at, (far, near) in enumerate(pairs)]
    ratings_copies = [
        pltpu.make_async_copy(far_ratings_ref.at[stripe], ratings_ref.at[stripe], ratings_sems.at[at])
        for at, stripe in enumerate(stripes)
    ]
    for copy in copies + ratings_copies:
        copy.start()
    for copy in copies:
        copy.wait()
    item = item_ref[...]
    side = (TILE, TILE)
    position = lax.broadcasted_iota(jnp.int32, side, 0) * TILE + lax.broadcasted_iota(jnp.int32, side, 1)

    def predicted_of(at):
        user = user_ref[:, stripes[at]]
        return lax.dot_general(user, item, (((0,), (0,)), ((), ())), preferred_element_type=jnp.float32)

    def add_share(at):
        share = jnp.dot(user_ref[:, stripes[at]], scaled_ref[stripes[at]], preferred_element_type=jnp.float32)
        if at > 0:
            share = share + total_ref[...]
        if at + 1 < len(stripes):
            total_ref[...] = share
        else:
            blocks = share.astype(jnp.bfloat16).reshape(item_share_ref.shape)
            first = SCATTER_FIRST * blocks.shape[0] // 16
            item_share_ref[...] = jnp.concatenate([blocks[first:], blocks[:first]]) if first else blocks

    predicted = predicted_of(0)
    errors = [jnp.zeros((8, TILE), jnp.float32)] * (columns // TILE)
    for at, start in enumerate(starts):
        ratings_copies[at].wait()
        following = predicted_of(at + 1) if at + 1 < len(stripes) else None
        for row in range(0, STRIPE, TILE):
            for column in range(0, columns, TILE):
                limit = limits_ref[column // TILE, (start + row) // TILE]
                rows, cols = pl.ds(start + row, TILE), pl.ds(column, TILE)
                rating = ratings_ref[rows, cols].astype(jnp.float32)
                difference = predicted[row : row + TILE, column : column + TILE] - rating
                residual = jnp.where(position < limit, difference, 0.0)
                scaled_ref[rows, cols] = residual.astype(jnp.bfloat16)
                error = (residual * residual).reshape(TILE // 8, 8, TILE).sum(axis=0)
                errors[column // TILE] = errors[column // TILE] + error
        if at > 0:
            add_share(at - 1)
        predicted = following
    add_share(len(stripes) - 1)
    error_ref[...] = jnp.concatenate(errors, axis=1)


def residual_of(limits, user, item, ratings, devices):
    rank, columns = item.shape
    flops = 4 * rank * ratings.size
    return pl.pallas_call(
        residual_body,
        in_specs=[FAR] * 4,
        out_specs=[VMEM] * 3,
        out_shape=[
            jax.ShapeDtypeStruct(ratings.shape, jnp.bfloat16),
            jax.ShapeDtypeStruct((devices, rank // devices, columns), jnp.bfloat16),
            jax.ShapeDtypeStruct((8, columns), jnp.float32),
        ],
        scratch_shapes=[
            pltpu.SMEM(limits.shape, jnp.int32),
            pltpu.VMEM(user.shape, jnp.bfloat16),
            pltpu.VMEM(item.shape, jnp.bfloat16),
            pltpu.VMEM(ratings.shape, jnp.bfloat16),
            pltpu.VMEM((rank, columns), jnp.float32),
            pltpu.SemaphoreType.DMA((4,)),
            pltpu.SemaphoreType.DMA((ratings.shape[0] // STRIPE,)),
        ],
        cost_estimate=pl.CostEstimate(flops=flops, bytes_accessed=4 * ratings.size, transcendentals=0),
        compiler_params=MOST_GRANT,
        name="residual",
    )(limits, user, item, ratings)


def user_share_body(layer_ref, item_ref, scaled_ref, mine_ref, other_ref):
    chips, height, _ = mine_ref.shape
    item = item_ref[...]
    first = layer_ref[0] == 0
    for start in range(0, scaled_ref.shape[0], STRIPE):
        stripe = pl.ds(start, STRIPE)
        share = lax.dot_general(item, scaled_ref[stripe], (((1,), (1,)), ((), ())), preferred_element_type=jnp.float32)
        share = share.reshape(chips, 2, height, STRIPE)
        for at in range(chips):
            even, odd = share[at, 0], share[at, 1]
            chip = (at - CHIP_FIRST * chips // 16) % chips
            mine_ref[chip, :, stripe] = jnp.where(first, even, odd).astype(jnp.bfloat16)
            other_ref[chip, :, stripe] = jnp.where(first, odd, even).astype(jnp.bfloat16)


def user_share_of(layer, item, scaled, height):
    shape = jax.ShapeDtypeStruct((item.shape[0] // height // 2, height, scaled.shape[0]), jnp.bfloat16)
    return pl.pallas_call(
        user_share_body,
        in_specs=[SMEM, VMEM, VMEM],
        out_specs=[VMEM, VMEM],
        out_shape=[shape, shape],
        cost_estimate=pl.CostEstimate(flops=2 * item.shape[0] * scaled.size, bytes_accessed=0, transcendentals=0),
        compiler_params=GRANT,
        name="user_share",
    )(layer, item, scaled)


def halves_body(mine_ref, arrived_ref, total_ref):
    total_ref[...] = (mine_ref[...].astype(jnp.float32) + arrived_ref[...].astype(jnp.float32)).astype(jnp.bfloat16)


def halves_summed(mine, arrived):
    return pl.pallas_call(
        halves_body,
        in_specs=[VMEM, VMEM],
        out_specs=VMEM,
        out_shape=jax.ShapeDtypeStruct(mine.shape, jnp.bfloat16),
        compiler_params=GRANT,
        name="halves",
    )(mine, arrived)


def summed(blocks_ref):
    total = blocks_ref[0].astype(jnp.float32)
    for i in range(1, blocks_ref.shape[0]):
        total = total + blocks_ref[i].astype(jnp.float32)
    return total


def item_raw_body(limits_ref, arrived_ref, user_ref, item_ref, error_ref, raw_ref, sums_ref):
    raw = summed(arrived_ref)
    raw_ref[...] = raw
    user, item = user_ref[...], item_ref[...]
    lane = lax.broadcasted_iota(jnp.int32, sums_ref.shape, 1)
    sums = jnp.zeros(sums_ref.shape, jnp.float32)
    for at, value in enumerate(
        (
            jnp.sum(limits_ref[...].astype(jnp.float32)),
            jnp.sum(user * user) + jnp.sum(item * item),
            jnp.sum(error_ref[...]),
            jnp.sum(raw * raw),
        )
    ):
        sums = jnp.where(lane == at, value, sums)
    sums_ref[...] = sums


def item_raw_of(limits, arrived, user_factor, item_factor, error):
    return pl.pallas_call(
        item_raw_body,
        in_specs=[VMEM] * 5,
        out_specs=[VMEM, VMEM],
        out_shape=[
            jax.ShapeDtypeStruct(arrived.shape[1:], jnp.float32),
            jax.ShapeDtypeStruct((1, LANES), jnp.float32),
        ],
        compiler_params=GRANT,
        name="item_raw",
    )(limits, arrived, user_factor, item_factor, error)


def user_raw_body(arrived_ref, sums_ref, raw_ref, packed_ref):
    raw = summed(arrived_ref)
    raw_ref[...] = raw
    lane = lax.broadcasted_iota(jnp.int32, sums_ref.shape, 1)
    sums = sums_ref[...] + jnp.where(lane == 3, jnp.sum(raw * raw), 0.0)
    packed_ref[...] = jnp.broadcast_to(sums[None], packed_ref.shape)


def user_raw_of(arrived, sums, devices):
    return pl.pallas_call(
        user_raw_body,
        in_specs=[VMEM, VMEM],
        out_specs=[VMEM, VMEM],
        out_shape=[
            jax.ShapeDtypeStruct(arrived.shape[1:], jnp.float32),
            jax.ShapeDtypeStruct((devices, *sums.shape), jnp.float32),
        ],
        compiler_params=GRANT,
        name="user_raw",
    )(arrived, sums)


def packed_again_body(arrived_ref, packed_ref):
    packed_ref[...] = jnp.broadcast_to(summed(arrived_ref)[None], packed_ref.shape)


def packed_again(arrived, devices):
    return pl.pallas_call(
        packed_again_body,
        in_specs=[VMEM],
        out_specs=VMEM,
        out_shape=jax.ShapeDtypeStruct((devices, *arrived.shape[1:]), jnp.float32),
        compiler_params=GRANT,
        name="packed_again",
    )(arrived)


def step_body(arrived_ref, user_ref, item_ref, raw_user_ref, raw_item_ref, new_user_ref, new_item_ref, loss_ref, norm_ref):
    sums = summed(arrived_ref)
    lane = lax.broadcasted_iota(jnp.int32, sums.shape, 1)

    def lane_at(at):
        return jnp.sum(jnp.where(lane == at, sums, 0.0), axis=1, keepdims=True)

    observed_total = jnp.maximum(lane_at(0), 1.0)
    scale = 2.0 / observed_total
    grad_norm = scale * jnp.sqrt(lane_at(3) + epsilon)
    step_size = trust_ratio * jnp.sqrt(lane_at(1) + epsilon) / grad_norm * scale
    new_user_ref[...] = user_ref[...] - step_size * raw_user_ref[...]
    new_item_ref[...] = item_ref[...] - step_size * raw_item_ref[...]
    loss_ref[0, 0] = jnp.sum(lane_at(2) / observed_total)
    norm_ref[0, 0] = jnp.sum(grad_norm)


def stepped(arrived, user_factor, item_factor, raw_user, raw_item):
    return pl.pallas_call(
        step_body,
        in_specs=[VMEM] * 5,
        out_specs=[VMEM, VMEM, SMEM, SMEM],
        out_shape=[
            jax.ShapeDtypeStruct(user_factor.shape, jnp.float32),
            jax.ShapeDtypeStruct(item_factor.shape, jnp.float32),
            jax.ShapeDtypeStruct((1, 1), jnp.float32),
            jax.ShapeDtypeStruct((1, 1), jnp.float32),
        ],
        compiler_params=GRANT,
        name="step",
    )(arrived, user_factor, item_factor, raw_user, raw_item)


def exchanged(blocks, axis, groups=None):
    return lax.all_to_all(blocks, axis, 0, 0, tiled=True, axis_index_groups=groups)


def listed_from(first, count):
    return [[(first + i) % count for i in range(count)]]


def shifted(array, axis, by):
    count = lax.axis_size(axis)
    return lax.ppermute(array, axis, [(i, (i + by) % count) for i in range(count)])


def body(ratings, tile_mask, tile_counts, user_factor, item_factor):
    rows, height = lax.axis_size("row"), user_factor.shape[0]
    devices, chips = lax.axis_size(COL_LAYER), lax.axis_size(("col_0", "col_1"))
    scatter_list, scalars_list = (listed_from(first * rows // 16, rows) for first in (SCATTER_FIRST, SCALARS_FIRST))
    chips_list, devices_list = (listed_from(CHIP_FIRST * count // 16, count) for count in (chips, devices))
    layer = lax.axis_index("layer").astype(jnp.int32)[None]
    user_blocks, limits = lowered_for_all(user_factor, tile_mask.T, tile_counts.T, devices)
    user = exchanged(user_blocks, COL_LAYER, devices_list).reshape(-1, user_factor.shape[1])
    item = lax.all_gather(item_factor.astype(jnp.bfloat16), "row", axis=0, tiled=True)
    scaled, item_share, error = residual_of(limits, user, item, ratings, rows)
    item_arrived = exchanged(item_share, "row", scatter_list)
    my_share, other_share = user_share_of(layer, item, scaled, height)
    partner_share = shifted(other_share, "layer", 1)
    halves = halves_summed(my_share, partner_share)
    user_arrived = exchanged(halves, ("col_0", "col_1"), chips_list)
    raw_item, sums = item_raw_of(limits, item_arrived, user_factor, item_factor, error)
    raw_user, packed = user_raw_of(user_arrived, sums, rows)
    packed = exchanged(packed, "row", scalars_list)
    packed = packed_again(packed, devices)
    packed = exchanged(packed, COL_LAYER, devices_list)
    new_user, new_item, loss_value, grad_norm = stepped(packed, user_factor, item_factor, raw_user, raw_item)
    return (new_user, new_item, loss_value.reshape(()), grad_norm.reshape(()))


def solution(mesh):
    finer = Mesh(
        mesh.devices.reshape(mesh.shape["row"], 4, 4, mesh.shape["layer"]),
        ("row", "col_0", "col_1", "layer"),
    )
    return jax.shard_map(
        body,
        mesh=finer,
        in_specs=(
            P("row", COL_LAYER),
            P("row", COL_LAYER),
            P("row", COL_LAYER),
            P(COL_LAYER, "row"),
            P("row", COL_LAYER),
        ),
        out_specs=(P(COL_LAYER, "row"), P("row", COL_LAYER), P(), P()),
        check_vma=False,
    )
```

```python
import jax
import jax.numpy as jnp
from jax import lax
from jax.experimental import pallas as pl
from jax.experimental.pallas import tpu as pltpu
from jax.sharding import Mesh
from jax.sharding import PartitionSpec as P

TILE = 128
LANES = 128
STRIPE = 512
SCATTER_FIRST, SCALARS_FIRST, CHIP_FIRST = 8, 8, 15
COL_LAYER = ("col_0", "col_1", "layer")
VMEM = pl.BlockSpec(memory_space=pltpu.VMEM)
SMEM = pl.BlockSpec(memory_space=pltpu.SMEM)
FAR = pl.BlockSpec(memory_space=pltpu.HBM)
GRANT = pltpu.CompilerParams(vmem_limit_bytes=16 * 2**20)
MOST_GRANT = pltpu.CompilerParams(vmem_limit_bytes=50 * 2**20)
WHOLE_GRANT = pltpu.CompilerParams(vmem_limit_bytes=60 * 2**20)

epsilon = 1e-12
trust_ratio = 0.2


def lower_body(user_ref, mask_ref, counts_ref, blocks_ref, limits_ref):
    user = user_ref[...].astype(jnp.bfloat16)
    blocks_ref[...] = jnp.broadcast_to(user[None], blocks_ref.shape)
    limits_ref[...] = jnp.where(mask_ref[...] == 1, counts_ref[...], 0)


def lowered_for_all(factor, mask, counts, devices):
    return pl.pallas_call(
        lower_body,
        in_specs=[VMEM] * 3,
        out_specs=[VMEM] * 2,
        out_shape=[
            jax.ShapeDtypeStruct((devices, *factor.shape), jnp.bfloat16),
            jax.ShapeDtypeStruct(mask.shape, jnp.int32),
        ],
        compiler_params=WHOLE_GRANT,
        name="lower",
    )(factor, mask, counts)


def residual_body(
    far_limits_ref, far_user_ref, far_item_ref, far_ratings_ref,
    scaled_ref, item_share_ref, error_ref,
    limits_ref, user_ref, item_ref, ratings_ref, total_ref, sems, ratings_sems,
):
    columns = ratings_ref.shape[1]
    starts = range(0, ratings_ref.shape[0], STRIPE)
    stripes = [pl.ds(start, STRIPE) for start in starts]
    rank = user_ref.shape[0]
    turn = CHIP_FIRST * rank // 16
    pairs = [
        (far_item_ref, item_ref),
        (far_limits_ref, limits_ref),
        (far_user_ref.at[pl.ds(0, rank - turn)], user_ref.at[pl.ds(turn, rank - turn)]),
        (far_user_ref.at[pl.ds(rank - turn, turn)], user_ref.at[pl.ds(0, turn)]),
    ]
    copies = [pltpu.make_async_copy(far, near, sems.at[at]) for at, (far, near) in enumerate(pairs)]
    ratings_copies = [
        pltpu.make_async_copy(far_ratings_ref.at[stripe], ratings_ref.at[stripe], ratings_sems.at[at])
        for at, stripe in enumerate(stripes)
    ]
    for copy in copies + ratings_copies:
        copy.start()
    for copy in copies:
        copy.wait()
    item = item_ref[...]
    side = (TILE, TILE)
    position = lax.broadcasted_iota(jnp.int32, side, 0) * TILE + lax.broadcasted_iota(jnp.int32, side, 1)

    def predicted_of(at):
        user = user_ref[:, stripes[at]]
        return lax.dot_general(user, item, (((0,), (0,)), ((), ())), preferred_element_type=jnp.float32)

    def add_share(at):
        share = jnp.dot(user_ref[:, stripes[at]], scaled_ref[stripes[at]], preferred_element_type=jnp.float32)
        if at > 0:
            share = share + total_ref[...]
        if at + 1 < len(stripes):
            total_ref[...] = share
        else:
            blocks = share.astype(jnp.bfloat16).reshape(item_share_ref.shape)
            first = SCATTER_FIRST * blocks.shape[0] // 16
            item_share_ref[...] = jnp.concatenate([blocks[first:], blocks[:first]]) if first else blocks

    predicted = predicted_of(0)
    errors = [jnp.zeros((8, TILE), jnp.float32)] * (columns // TILE)
    for at, start in enumerate(starts):
        ratings_copies[at].wait()
        following = predicted_of(at + 1) if at + 1 < len(stripes) else None
        for row in range(0, STRIPE, TILE):
            for column in range(0, columns, TILE):
                limit = limits_ref[column // TILE, (start + row) // TILE]
                rows, cols = pl.ds(start + row, TILE), pl.ds(column, TILE)
                rating = ratings_ref[rows, cols].astype(jnp.float32)
                difference = predicted[row : row + TILE, column : column + TILE] - rating
                residual = jnp.where(position < limit, difference, 0.0)
                scaled_ref[rows, cols] = residual.astype(jnp.bfloat16)
                error = (residual * residual).reshape(TILE // 8, 8, TILE).sum(axis=0)
                errors[column // TILE] = errors[column // TILE] + error
        if at > 0:
            add_share(at - 1)
        predicted = following
    add_share(len(stripes) - 1)
    error_ref[...] = jnp.concatenate(errors, axis=1)


def residual_of(limits, user, item, ratings, devices):
    rank, columns = item.shape
    flops = 4 * rank * ratings.size
    return pl.pallas_call(
        residual_body,
        in_specs=[FAR] * 4,
        out_specs=[VMEM] * 3,
        out_shape=[
            jax.ShapeDtypeStruct(ratings.shape, jnp.bfloat16),
            jax.ShapeDtypeStruct((devices, rank // devices, columns), jnp.bfloat16),
            jax.ShapeDtypeStruct((8, columns), jnp.float32),
        ],
        scratch_shapes=[
            pltpu.SMEM(limits.shape, jnp.int32),
            pltpu.VMEM(user.shape, jnp.bfloat16),
            pltpu.VMEM(item.shape, jnp.bfloat16),
            pltpu.VMEM(ratings.shape, jnp.bfloat16),
            pltpu.VMEM((rank, columns), jnp.float32),
            pltpu.SemaphoreType.DMA((4,)),
            pltpu.SemaphoreType.DMA((ratings.shape[0] // STRIPE,)),
        ],
        cost_estimate=pl.CostEstimate(flops=flops, bytes_accessed=4 * ratings.size, transcendentals=0),
        compiler_params=MOST_GRANT,
        name="residual",
    )(limits, user, item, ratings)


def user_share_body(layer_ref, item_ref, scaled_ref, mine_ref, other_ref):
    chips, height, _ = mine_ref.shape
    item = item_ref[...]
    first = layer_ref[0] == 0
    for start in range(0, scaled_ref.shape[0], STRIPE):
        stripe = pl.ds(start, STRIPE)
        share = lax.dot_general(item, scaled_ref[stripe], (((1,), (1,)), ((), ())), preferred_element_type=jnp.float32)
        share = share.reshape(chips, 2, height, STRIPE)
        for at in range(chips):
            even, odd = share[at, 0], share[at, 1]
            chip = (at - CHIP_FIRST * chips // 16) % chips
            mine_ref[chip, :, stripe] = jnp.where(first, even, odd).astype(jnp.bfloat16)
            other_ref[chip, :, stripe] = jnp.where(first, odd, even).astype(jnp.bfloat16)


def user_share_of(layer, item, scaled, height):
    shape = jax.ShapeDtypeStruct((item.shape[0] // height // 2, height, scaled.shape[0]), jnp.bfloat16)
    return pl.pallas_call(
        user_share_body,
        in_specs=[SMEM, VMEM, VMEM],
        out_specs=[VMEM, VMEM],
        out_shape=[shape, shape],
        cost_estimate=pl.CostEstimate(flops=2 * item.shape[0] * scaled.size, bytes_accessed=0, transcendentals=0),
        compiler_params=GRANT,
        name="user_share",
    )(layer, item, scaled)


def halves_body(mine_ref, arrived_ref, total_ref):
    total_ref[...] = (mine_ref[...].astype(jnp.float32) + arrived_ref[...].astype(jnp.float32)).astype(jnp.bfloat16)


def halves_summed(mine, arrived):
    return pl.pallas_call(
        halves_body,
        in_specs=[VMEM, VMEM],
        out_specs=VMEM,
        out_shape=jax.ShapeDtypeStruct(mine.shape, jnp.bfloat16),
        compiler_params=GRANT,
        name="halves",
    )(mine, arrived)


def summed(blocks_ref):
    total = blocks_ref[0].astype(jnp.float32)
    for i in range(1, blocks_ref.shape[0]):
        total = total + blocks_ref[i].astype(jnp.float32)
    return total


def item_raw_body(limits_ref, arrived_ref, user_ref, item_ref, error_ref, raw_ref, sums_ref):
    raw = summed(arrived_ref)
    raw_ref[...] = raw
    user, item = user_ref[...], item_ref[...]
    lane = lax.broadcasted_iota(jnp.int32, sums_ref.shape, 1)
    sums = jnp.zeros(sums_ref.shape, jnp.float32)
    for at, value in enumerate(
        (
            jnp.sum(limits_ref[...].astype(jnp.float32)),
            jnp.sum(user * user) + jnp.sum(item * item),
            jnp.sum(error_ref[...]),
            jnp.sum(raw * raw),
        )
    ):
        sums = jnp.where(lane == at, value, sums)
    sums_ref[...] = sums


def item_raw_of(limits, arrived, user_factor, item_factor, error):
    return pl.pallas_call(
        item_raw_body,
        in_specs=[VMEM] * 5,
        out_specs=[VMEM, VMEM],
        out_shape=[
            jax.ShapeDtypeStruct(arrived.shape[1:], jnp.float32),
            jax.ShapeDtypeStruct((1, LANES), jnp.float32),
        ],
        compiler_params=GRANT,
        name="item_raw",
    )(limits, arrived, user_factor, item_factor, error)


def user_raw_body(arrived_ref, sums_ref, raw_ref, packed_ref):
    raw = summed(arrived_ref)
    raw_ref[...] = raw
    lane = lax.broadcasted_iota(jnp.int32, sums_ref.shape, 1)
    sums = sums_ref[...] + jnp.where(lane == 3, jnp.sum(raw * raw), 0.0)
    packed_ref[...] = jnp.broadcast_to(sums[None], packed_ref.shape)


def user_raw_of(arrived, sums, devices):
    return pl.pallas_call(
        user_raw_body,
        in_specs=[VMEM, VMEM],
        out_specs=[VMEM, VMEM],
        out_shape=[
            jax.ShapeDtypeStruct(arrived.shape[1:], jnp.float32),
            jax.ShapeDtypeStruct((devices, *sums.shape), jnp.float32),
        ],
        compiler_params=GRANT,
        name="user_raw",
    )(arrived, sums)


def packed_again_body(arrived_ref, packed_ref):
    packed_ref[...] = jnp.broadcast_to(summed(arrived_ref)[None], packed_ref.shape)


def packed_again(arrived, devices):
    return pl.pallas_call(
        packed_again_body,
        in_specs=[VMEM],
        out_specs=VMEM,
        out_shape=jax.ShapeDtypeStruct((devices, *arrived.shape[1:]), jnp.float32),
        compiler_params=GRANT,
        name="packed_again",
    )(arrived)


def step_body(arrived_ref, user_ref, item_ref, raw_user_ref, raw_item_ref, new_user_ref, new_item_ref, loss_ref, norm_ref):
    sums = summed(arrived_ref)
    lane = lax.broadcasted_iota(jnp.int32, sums.shape, 1)

    def lane_at(at):
        return jnp.sum(jnp.where(lane == at, sums, 0.0), axis=1, keepdims=True)

    observed_total = jnp.maximum(lane_at(0), 1.0)
    scale = 2.0 / observed_total
    grad_norm = scale * jnp.sqrt(lane_at(3) + epsilon)
    step_size = trust_ratio * jnp.sqrt(lane_at(1) + epsilon) / grad_norm * scale
    new_user_ref[...] = user_ref[...] - step_size * raw_user_ref[...]
    new_item_ref[...] = item_ref[...] - step_size * raw_item_ref[...]
    loss_ref[0, 0] = jnp.sum(lane_at(2) / observed_total)
    norm_ref[0, 0] = jnp.sum(grad_norm)


def stepped(arrived, user_factor, item_factor, raw_user, raw_item):
    return pl.pallas_call(
        step_body,
        in_specs=[VMEM] * 5,
        out_specs=[VMEM, VMEM, SMEM, SMEM],
        out_shape=[
            jax.ShapeDtypeStruct(user_factor.shape, jnp.float32),
            jax.ShapeDtypeStruct(item_factor.shape, jnp.float32),
            jax.ShapeDtypeStruct((1, 1), jnp.float32),
            jax.ShapeDtypeStruct((1, 1), jnp.float32),
        ],
        compiler_params=GRANT,
        name="step",
    )(arrived, user_factor, item_factor, raw_user, raw_item)


def exchanged(blocks, axis, groups=None):
    return lax.all_to_all(blocks, axis, 0, 0, tiled=True, axis_index_groups=groups)


def listed_from(first, count):
    return [[(first + i) % count for i in range(count)]]


def shifted(array, axis, by):
    count = lax.axis_size(axis)
    return lax.ppermute(array, axis, [(i, (i + by) % count) for i in range(count)])


def body(ratings, tile_mask, tile_counts, user_factor, item_factor):
    rows, height = lax.axis_size("row"), user_factor.shape[0]
    devices, chips = lax.axis_size(COL_LAYER), lax.axis_size(("col_0", "col_1"))
    scatter_list, scalars_list = (listed_from(first * rows // 16, rows) for first in (SCATTER_FIRST, SCALARS_FIRST))
    chips_list, devices_list = (listed_from(CHIP_FIRST * count // 16, count) for count in (chips, devices))
    layer = lax.axis_index("layer").astype(jnp.int32)[None]
    user_blocks, limits = lowered_for_all(user_factor, tile_mask.T, tile_counts.T, devices)
    user = exchanged(user_blocks, COL_LAYER, devices_list).reshape(-1, user_factor.shape[1])
    item = lax.all_gather(item_factor.astype(jnp.bfloat16), "row", axis=0, tiled=True)
    scaled, item_share, error = residual_of(limits, user, item, ratings, rows)
    item_arrived = exchanged(item_share, "row", scatter_list)
    my_share, other_share = user_share_of(layer, item, scaled, height)
    partner_share = shifted(other_share, "layer", 1)
    halves = halves_summed(my_share, partner_share)
    user_arrived = exchanged(halves, ("col_0", "col_1"), chips_list)
    raw_item, sums = item_raw_of(limits, item_arrived, user_factor, item_factor, error)
    raw_user, packed = user_raw_of(user_arrived, sums, devices)
    packed = exchanged(packed, COL_LAYER, devices_list)
    packed = packed_again(packed, rows)
    packed = exchanged(packed, "row", scalars_list)
    new_user, new_item, loss_value, grad_norm = stepped(packed, user_factor, item_factor, raw_user, raw_item)
    return (new_user, new_item, loss_value.reshape(()), grad_norm.reshape(()))


def solution(mesh):
    finer = Mesh(
        mesh.devices.reshape(mesh.shape["row"], 4, 4, mesh.shape["layer"]),
        ("row", "col_0", "col_1", "layer"),
    )
    return jax.shard_map(
        body,
        mesh=finer,
        in_specs=(
            P("row", COL_LAYER),
            P("row", COL_LAYER),
            P("row", COL_LAYER),
            P(COL_LAYER, "row"),
            P("row", COL_LAYER),
        ),
        out_specs=(P(COL_LAYER, "row"), P("row", COL_LAYER), P(), P()),
        check_vma=False,
    )
```
